32 devices in a mesh: gx: 4 (over x, core), gy: 8 (over z, y).
Axes of the slice: x: 2, y: 2, z: 4, core: 2. Of those that a mesh axis runs over, the one named last changes fastest.
Arguments:
- fine_start: float32 [3, 1024, 4096], P(None, 'gx', 'gy'), may hold values from -6 to 6
- fine_known: float32 [3, 1024, 4096], P(None, 'gx', 'gy'), may hold values from -18 to 18
- fine_mu: float32 [1024, 4096], P('gx', 'gy'), may hold values from 1 to 10
- coarse_start: float32 [3, 512, 2048], P(None, ('gx', 'gy')), may hold values from -6 to 6
- coarse_known: float32 [3, 512, 2048], P(None, ('gx', 'gy')), may hold values from -18 to 18
- coarse_mu: float32 [512, 2048], P(('gx', 'gy')), may hold values from 1 to 10
Outputs:
- fine_ghost: float32 [3, 1024, 4096], P(None, 'gx', 'gy')
- coarse_ghost: float32 [3, 512, 2048], P(None, ('gx', 'gy'))
- norms: float32 [3], replicated
The draws below stay inside these ranges and needn't reach their ends.
All inputs are finite; a program needn't handle non-finite values.
Results may differ from the reference program's by a relative error of at most 0.0001.
Values sent between devices are 32-bit elements; how exact they have to be, the bound alone decides.
A program may use at most 128 MiB of HBM per device.

```python
import math
import jax
import jax.numpy as jnp

ITERS = 3
NCX = 512
NCY = 2048
NFX = 1024
NFY = 4096


def rising_field(key, rows, cols):
    ramp = 1.0 + 2.0 * jnp.arange(rows, dtype=jnp.float32)[:, None] / max(rows - 1, 1)
    base = jnp.clip(jax.random.normal(key, (3, rows, cols), jnp.float32), -6.0, 6.0)
    return base * ramp[None]


def draw_fine_known(key, part):
    return rising_field(jax.random.fold_in(key, 11), NFX, NFY)


def draw_coarse_known(key, part):
    return rising_field(jax.random.fold_in(key, 23), NCX, NCY)


def steps_of(stream_key, extent, split, least, top_value):
    def one(dim, blocks):
        steps = jax.random.uniform(jax.random.fold_in(jax.random.fold_in(stream_key, 6), dim), (blocks,), jnp.float32, least / len(split), top_value / len(split))
        return jnp.repeat(jnp.exp(steps), extent[dim] // blocks).reshape((-1,) + (1,) * (len(extent) - dim - 1))

    gain = one(*split[0])
    for cut in split[1:]:
        gain = gain * one(*cut)
    return gain


def bell_draw(key, extent, spread, limit, split=(), kind=jnp.bfloat16):
    factor_of = steps_of(key, extent, split, -0.22, 0.18) if split else 1.0
    drawn = jax.random.normal(key, extent, jnp.float32) * spread * factor_of
    return jnp.minimum(jnp.maximum(drawn, -limit), limit).astype(kind)


def setup_inputs(seed: int = 0) -> dict:
    arg_keys = jax.random.split(jax.random.key(seed), 7)
    return {
        "fine_start": bell_draw(arg_keys[0], (3, NFX, NFY), 1.0, 6.0, ((1, 4), (2, 8)), jnp.float32),
        "fine_known": draw_fine_known(jax.random.fold_in(arg_keys[6], 71), 0),
        "fine_mu": jnp.clip(jnp.exp(math.log(10.0) - 2.3025851 * jax.random.uniform(arg_keys[2], (NFX, NFY), jnp.float32) ** steps_of(arg_keys[2], (NFX, NFY), ((0, 4), (1, 8)), -0.2, 0.2)), 1.0, 10.0),
        "coarse_start": bell_draw(arg_keys[3], (3, NCX, NCY), 1.0, 6.0, ((1, 32),), jnp.float32),
        "coarse_known": draw_coarse_known(jax.random.fold_in(arg_keys[6], 71), 0),
        "coarse_mu": jnp.clip(jnp.exp(math.log(10.0) - 2.3025851 * jax.random.uniform(arg_keys[5], (NCX, NCY), jnp.float32) ** steps_of(arg_keys[5], (NCX, NCY), ((0, 32),), -0.2, 0.2)), 1.0, 10.0),
    }


def neighbours(padded):
    return padded[:, 2:, 1:-1] + padded[:, :-2, 1:-1] + padded[:, 1:-1, 2:] + padded[:, 1:-1, :-2]

def prolong(padded):
    components, rows_plus, cols_plus = padded.shape
    middle = padded[:, 1:-1, :]
    even_rows = 0.75 * middle + 0.25 * padded[:, :-2, :]
    odd_rows = 0.75 * middle + 0.25 * padded[:, 2:, :]
    row_fine = jnp.stack([even_rows, odd_rows], axis=2).reshape(components, 2 * (rows_plus - 2), cols_plus)
    centre = row_fine[:, :, 1:-1]
    even_cols = 0.75 * centre + 0.25 * row_fine[:, :, :-2]
    odd_cols = 0.75 * centre + 0.25 * row_fine[:, :, 2:]
    return jnp.stack([even_cols, odd_cols], axis=3).reshape(components, 2 * (rows_plus - 2), 2 * (cols_plus - 2))

def restrict(fine):
    return 0.25 * (fine[:, 0::2, 0::2] + fine[:, 1::2, 0::2] + fine[:, 0::2, 1::2] + fine[:, 1::2, 1::2])

def pad_plane(field):
    return jnp.pad(field, ((0, 0), (1, 1), (1, 1)))

def reference(fine_start, fine_known, fine_mu, coarse_start, coarse_known, coarse_mu):
    fine_diag = (fine_mu + 1.0)[None]
    coarse_diag = (coarse_mu + 1.0)[None]
    fine_ghost = fine_start
    coarse_ghost = coarse_start
    cell_total = 3.0 * (NFX * NFY + NCX * NCY)
    norm_list = []
    for sweep in range(ITERS):
        coarse_padded = pad_plane(coarse_ghost)
        fine_res = fine_known + 0.25 * neighbours(pad_plane(fine_ghost)) + 0.5 * prolong(coarse_padded) - fine_diag * fine_ghost
        coarse_res = coarse_known + 0.25 * neighbours(coarse_padded) + 0.5 * restrict(fine_ghost) - coarse_diag * coarse_ghost
        total = jnp.sum(fine_res * fine_res) + jnp.sum(coarse_res * coarse_res)
        norm_list.append(jnp.sqrt(total / cell_total))
        fine_ghost = fine_ghost + fine_res / fine_diag
        coarse_ghost = coarse_ghost + coarse_res / coarse_diag
    return (fine_ghost, coarse_ghost, jnp.stack(norm_list))
```

```python
import functools

import jax
import jax.numpy as jnp
from jax import lax
from jax.experimental import pallas as pl
from jax.experimental.pallas import tpu as pltpu
from jax.sharding import PartitionSpec as P

ITERS = 3
LANES = 128
SUB = 8
MESH = pl.DeviceIdType.MESH
DIRECTIONS = ((-1, 0), (1, 0), (0, -1), (0, 1), (-1, -1), (1, 1), (-1, 1), (1, -1))


def lane_index():
    return lax.broadcasted_iota(jnp.int32, (SUB, LANES), 1)


def roll_lanes(cells, shift):
    shift = shift % LANES
    return cells if shift == 0 else pltpu.roll(cells, shift, 1)


def from_left(halves, halo):
    first = lane_index() == 0
    rolled = [roll_lanes(cells, 1) for cells in halves]
    return [jnp.where(first, before, own) for before, own in zip([halo] + rolled[:-1], rolled)]


def from_right(halves, halo):
    last = lane_index() == LANES - 1
    rolled = [roll_lanes(cells, LANES - 1) for cells in halves]
    return [jnp.where(last, after, own) for own, after in zip(rolled, rolled[1:] + [halo])]


def kernel(
    n_gx,
    n_gy,
    cells_total,
    fine_start,
    fine_known,
    fine_mu,
    coarse_start,
    coarse_known,
    coarse_mu,
    fine_out,
    coarse_out,
    norms_out,
    raw_start,
    raw_known,
    raw_mu,
    fine,
    known,
    diag,
    inverse,
    patch_start,
    patch_known,
    patch_mu,
    coarse,
    patch_out,
    row_send,
    col_send,
    col_out,
    row_recv,
    col_recv,
    corner_recv,
    left_halo,
    right_halo,
    norm_x,
    norm_y,
    load_sem,
    store_sem,
    own_sem,
    move_send,
    move_recv,
    halo_send,
    halo_recv,
    back_own,
    back_send,
    back_recv,
    normx_send,
    normx_recv,
    normy_send,
    normy_recv,
):
    gx = lax.axis_index("gx")
    gy = lax.axis_index("gy")
    comps, rows, width = patch_start.shape
    halves = width // LANES
    blocks = rows // SUB
    own_rows = coarse_start.shape[1]
    lane = lane_index()

    loads = []
    for which, (source, target) in enumerate(
        ((fine_start, raw_start), (fine_mu, raw_mu), (fine_known, raw_known))
    ):
        for tile in range(2 * halves):
            at = pl.ds(tile * LANES, LANES)
            view = source.at[:, at] if len(source.shape) == 2 else source.at[:, :, at]
            loads.append(
                pltpu.make_async_copy(view, target.at[tile], load_sem.at[which, tile])
            )
    for copy in loads:
        copy.start()

    row_recv[...] = jnp.zeros_like(row_recv)
    col_recv[...] = jnp.zeros_like(col_recv)
    corner_recv[...] = jnp.zeros_like(corner_recv)
    col_send[...] = jnp.zeros_like(col_send)
    row_send[...] = jnp.zeros_like(row_send)

    barrier = pltpu.get_barrier_semaphore()

    def greet_gy(step, carry):
        pl.semaphore_signal(
            barrier, inc=1, device_id={"gy": lax.rem(gy + step, n_gy)}, device_id_type=MESH
        )
        return carry

    def greet_gx(step, carry):
        pl.semaphore_signal(
            barrier, inc=1, device_id={"gx": lax.rem(gx + step, n_gx)}, device_id_type=MESH
        )
        return carry

    lax.fori_loop(1, n_gy, greet_gy, 0)
    lax.fori_loop(1, n_gx, greet_gx, 0)

    def inside(direction):
        dx, dy = DIRECTIONS[direction]
        checks = []
        if dx:
            checks.append(gx > 0 if dx < 0 else gx < n_gx - 1)
        if dy:
            checks.append(gy > 0 if dy < 0 else gy < n_gy - 1)
        return functools.reduce(jnp.logical_and, checks)

    for direction in range(4, 8):
        dx, dy = DIRECTIONS[direction]

        @pl.when(inside(direction))
        def _():
            pl.semaphore_signal(
                barrier, inc=1, device_id={"gx": gx + dx, "gy": gy + dy}, device_id_type=MESH
            )

    sides_x = (gx > 0).astype(jnp.int32) + (gx < n_gx - 1).astype(jnp.int32)
    sides_y = (gy > 0).astype(jnp.int32) + (gy < n_gy - 1).astype(jnp.int32)
    pl.semaphore_wait(barrier, n_gy - 1 + n_gx - 1 + sides_x * sides_y)

    moved = ((coarse_start, patch_start), (coarse_known, patch_known), (coarse_mu, patch_mu))

    def move(which, owner, place, sem):
        source, target = moved[which]
        columns = pl.ds(pl.multiple_of(owner * width, LANES), width)
        lines = pl.ds(pl.multiple_of(place * own_rows, SUB), own_rows)
        if len(source.shape) == 2:
            return source.at[:, columns], target.at[lines, :]
        return source.at[:, :, columns], target.at[:, lines, :]

    def own_move(which):
        source, target = move(which, gy, gy, None)
        return pltpu.make_async_copy(source, target, own_sem.at[which])

    def peer_move(which, step):
        peer = lax.rem(gy + step, n_gy)
        source, target = move(which, peer, gy, None)
        return pltpu.make_async_remote_copy(
            source,
            target,
            move_send.at[which, step],
            move_recv.at[which, step],
            device_id={"gy": peer},
            device_id_type=MESH,
        )

    def wait_moves(which):
        own_move(which).wait()

        def body(step, carry):
            peer = lax.rem(gy + n_gy - step, n_gy)
            source, target = move(which, gy, peer, None)
            pltpu.make_async_remote_copy(
                source,
                target,
                move_send.at[which, step],
                move_recv.at[which, step],
                device_id={"gy": lax.rem(gy + step, n_gy)},
                device_id_type=MESH,
            ).wait()
            return carry

        lax.fori_loop(1, n_gy, body, 0)

    for which in range(3):

        def send_step(step, carry, which=which):
            peer_move(which, step).start()
            return carry

        lax.fori_loop(1, n_gy, send_step, 0)
        own_move(which).start()

    half_lane = lane < LANES // 2
    evens_first = jnp.where(half_lane, 2 * lane, 2 * lane - LANES + 1)
    odds_first = jnp.where(half_lane, 2 * lane + 1, 2 * lane - LANES)

    def split_columns(a, b):
        a = jnp.take_along_axis(a, evens_first, axis=1)
        b = jnp.take_along_axis(b, odds_first, axis=1)
        return (
            jnp.where(half_lane, a, b),
            pltpu.roll(jnp.where(half_lane, b, a), LANES // 2, 1),
        )

    def split_field(raw, put):
        def body(i, carry):
            comp, block = i // blocks, i % blocks
            for parity in range(2):
                for half in range(halves):
                    at = pl.ds(block * 2 * SUB + parity, SUB, stride=2)
                    even, odd = split_columns(
                        raw[2 * half, comp, at, :], raw[2 * half + 1, comp, at, :]
                    )
                    put(comp, parity, 0, half, block, even)
                    put(comp, parity, 1, half, block, odd)
            return carry

        lax.fori_loop(0, comps * blocks, body, 0)

    def rows_of(block, shift=0):
        if shift == 0:
            return pl.ds(pl.multiple_of(block * SUB + SUB, SUB), SUB)
        return pl.ds(block * SUB + SUB + shift, SUB)

    def plain(block):
        return pl.ds(pl.multiple_of(block * SUB, SUB), SUB)

    def put_start(comp, parity, side, half, block, cells):
        fine[0, comp, parity, side, half, rows_of(block), :] = cells

    def put_known(comp, parity, side, half, block, cells):
        known[comp, parity, side, half, plain(block), :] = cells

    def split_mu(block, carry):
        for parity in range(2):
            for half in range(halves):
                at = pl.ds(block * 2 * SUB + parity, SUB, stride=2)
                both = split_columns(raw_mu[2 * half, at, :], raw_mu[2 * half + 1, at, :])
                for side in range(2):
                    total = both[side] + 1.0
                    diag[parity, side, half, plain(block), :] = total
                    inverse[parity, side, half, plain(block), :] = 1.0 / total
        return carry

    tiles = 2 * halves
    for copy in loads[:tiles]:
        copy.wait()
    split_field(raw_start, put_start)
    for copy in loads[tiles : 2 * tiles]:
        copy.wait()
    lax.fori_loop(0, blocks, split_mu, 0)
    for copy in loads[2 * tiles :]:
        copy.wait()
    split_field(raw_known, put_known)

    wait_moves(0)

    def place_start(i, carry):
        comp, block = i // blocks, i % blocks
        for half in range(halves):
            coarse[0, comp, half, rows_of(block), :] = patch_start[
                comp, plain(block), half * LANES : (half + 1) * LANES
            ]
        return carry

    lax.fori_loop(0, comps * blocks, place_start, 0)

    def exchange(sweep, buf):
        for way, (parity, line) in enumerate(((0, SUB), (1, SUB + rows - 1))):
            for half in range(halves):
                for comp in range(comps):
                    for side in range(2):
                        at = 2 * comp + side
                        row_send[sweep, way, half, at : at + 1, :] = fine[
                            buf, comp, parity, side, half, line : line + 1, :
                        ]
                    row_send[sweep, way, half, SUB + comp : SUB + comp + 1, :] = coarse[
                        buf, comp, half, line : line + 1, :
                    ]

        def gather(block, carry):
            for way, (half, at, side) in enumerate(((0, 0, 0), (halves - 1, LANES - 1, 1))):
                cells = jnp.zeros((SUB, LANES), jnp.float32)
                for k in range(3 * comps):
                    if k < 2 * comps:
                        edge = fine[buf, k // 2, k % 2, side, half, rows_of(block), :]
                    else:
                        edge = coarse[buf, k - 2 * comps, half, rows_of(block), :]
                    cells = jnp.where(lane == k, roll_lanes(edge, k - at), cells)
                col_send[way, plain(block), :] = cells
            return carry

        lax.fori_loop(0, blocks, gather, 0)
        for way in range(2):
            turned = col_send[way, :, :].T
            col_turned = turned[: 2 * SUB]
            col_out[sweep, way, :, :] = col_turned

        def message(direction):
            dx, dy = DIRECTIONS[direction]
            way = direction % 2
            if direction < 2:
                source, target = row_send.at[sweep, way], row_recv.at[sweep, 1 - way]
            elif direction < 4:
                source = col_out.at[sweep, way]
                target = col_recv.at[sweep, 1 - way, pl.ds(0, 2 * SUB), :]
            else:
                half = 0 if dy < 0 else halves - 1
                source = row_send.at[sweep, 0 if dx < 0 else 1, half, pl.ds(SUB, SUB), :]
                target = corner_recv.at[sweep, (direction ^ 1) - 4]
            return pltpu.make_async_remote_copy(
                source,
                target,
                halo_send.at[sweep, direction],
                halo_recv.at[sweep, direction ^ 1],
                device_id={"gx": gx + dx, "gy": gy + dy},
                device_id_type=MESH,
            )

        for direction in range(8):

            @pl.when(inside(direction))
            def _():
                message(direction).start()

        for direction in range(8):

            @pl.when(inside(direction))
            def _():
                message(direction).wait_send()
                message(direction ^ 1).wait_recv()

        for half in range(halves):
            for comp in range(comps):
                for side in range(2):
                    at = 2 * comp + side
                    fine[buf, comp, 1, side, half, SUB - 1 : SUB, :] = row_recv[
                        sweep, 0, half, at : at + 1, :
                    ]
                    fine[buf, comp, 0, side, half, SUB + rows : SUB + rows + 1, :] = row_recv[
                        sweep, 1, half, at : at + 1, :
                    ]
                for way, line in enumerate((SUB - 1, SUB + rows)):
                    coarse[buf, comp, half, line : line + 1, :] = row_recv[
                        sweep, way, half, SUB + comp : SUB + comp + 1, :
                    ]
        left_halo[SUB : SUB + rows, :] = col_recv[sweep, 0].T
        right_halo[SUB : SUB + rows, :] = col_recv[sweep, 1].T
        for target, corners, at in ((left_halo, (0, 3), LANES - 1), (right_halo, (2, 1), 0)):
            for corner, line in zip(corners, (SUB - 1, SUB + rows)):
                block = corner_recv[sweep, corner]
                held = jnp.zeros((SUB, LANES), jnp.float32)
                for comp in range(comps):
                    k = 2 * comps + comp
                    held = jnp.where(
                        lane == k, roll_lanes(pltpu.roll(block, (SUB - comp) % SUB, 0)
                                              if comp else block, k - at), held
                    )
                target[line : line + 1, :] = held[0:1, :]

    def halo_pair(k, lines):
        left = pltpu.roll(left_halo[lines, :], lax.rem(LANES - k, LANES), 1)
        right = pltpu.roll(right_halo[lines, :], lax.rem(LANES - 1 - k, LANES), 1)
        return left, right

    def coarse_pass(buf, last):
        def body(i, total):
            comp, block = i // blocks, i % blocks
            k = 2 * comps + comp
            left, right = halo_pair(k, rows_of(block))
            own = [coarse[buf, comp, half, rows_of(block), :] for half in range(halves)]
            lefts, rights = from_left(own, left), from_right(own, right)
            for half in range(halves):
                columns = slice(half * LANES, (half + 1) * LANES)
                near = (
                    coarse[buf, comp, half, rows_of(block, 1), :]
                    + coarse[buf, comp, half, rows_of(block, -1), :]
                    + rights[half]
                    + lefts[half]
                )
                below = (
                    fine[buf, comp, 0, 0, half, rows_of(block), :]
                    + fine[buf, comp, 1, 0, half, rows_of(block), :]
                    + fine[buf, comp, 0, 1, half, rows_of(block), :]
                    + fine[buf, comp, 1, 1, half, rows_of(block), :]
                )
                scale = patch_mu[plain(block), columns] + 1.0
                res = (
                    patch_known[comp, plain(block), columns]
                    + 0.25 * near
                    + 0.125 * below
                    - scale * own[half]
                )
                total = total + res * res
                new = own[half] + res / scale
                if last:
                    patch_out[comp, plain(block), columns] = new
                else:
                    coarse[1 - buf, comp, half, rows_of(block), :] = new
            return total

        return lax.fori_loop(0, comps * blocks, body, jnp.zeros((SUB, LANES), jnp.float32))

    def fine_pass(buf):
        def body(i, total):
            comp, block = i // blocks, i % blocks
            k = 2 * comps + comp
            mid = [coarse[buf, comp, half, rows_of(block), :] for half in range(halves)]
            mid_left, mid_right = halo_pair(k, rows_of(block))
            for parity in range(2):
                shift = 1 if parity else -1
                far_left, far_right = halo_pair(k, rows_of(block, shift))
                line = [
                    0.75 * mid[half]
                    + 0.25 * coarse[buf, comp, half, rows_of(block, shift), :]
                    for half in range(halves)
                ]
                line_left = from_left(line, 0.75 * mid_left + 0.25 * far_left)
                line_right = from_right(line, 0.75 * mid_right + 0.25 * far_right)
                fine_left, fine_right = halo_pair(2 * comp + parity, rows_of(block))
                evens = [fine[buf, comp, parity, 0, half, rows_of(block), :] for half in range(halves)]
                odds = [fine[buf, comp, parity, 1, half, rows_of(block), :] for half in range(halves)]
                before, after = from_left(odds, fine_left), from_right(evens, fine_right)
                for half in range(halves):
                    for side in range(2):
                        own = odds[half] if side else evens[half]
                        lateral = (
                            evens[half] + after[half] if side else odds[half] + before[half]
                        )
                        near = (
                            fine[buf, comp, 1 - parity, side, half, rows_of(block), :]
                            + fine[buf, comp, 1 - parity, side, half, rows_of(block, shift), :]
                            + lateral
                        )
                        spread = 0.75 * line[half] + 0.25 * (
                            line_right[half] if side else line_left[half]
                        )
                        res = (
                            known[comp, parity, side, half, plain(block), :]
                            + 0.25 * near
                            + 0.5 * spread
                            - diag[parity, side, half, plain(block), :] * own
                        )
                        total = total + res * res
                        fine[1 - buf, comp, parity, side, half, rows_of(block), :] = (
                            own + res * inverse[parity, side, half, plain(block), :]
                        )
            return total

        return lax.fori_loop(0, comps * blocks, body, jnp.zeros((SUB, LANES), jnp.float32))

    def back_place(owner, place):
        return (
            patch_out.at[:, pl.ds(pl.multiple_of(owner * own_rows, SUB), own_rows), :],
            coarse_out.at[:, :, pl.ds(pl.multiple_of(place * width, LANES), width)],
        )

    def back_move(step, place_step):
        peer = lax.rem(gy + step, n_gy)
        source, _ = back_place(peer, gy)
        _, target = back_place(peer, lax.rem(gy + place_step, n_gy))
        return pltpu.make_async_remote_copy(
            source,
            target,
            back_send.at[step],
            back_recv.at[step],
            device_id={"gy": peer},
            device_id_type=MESH,
        )

    def back_start(step, carry):
        back_move(step, 0).start()
        return carry

    def back_wait(step, carry):
        back_move(step, n_gy - step).wait()
        return carry

    own_back = pltpu.make_async_copy(*back_place(gy, gy), back_own.at[0])
    row = lax.broadcasted_iota(jnp.int32, (SUB, LANES), 0)
    sums = jnp.zeros((SUB, LANES), jnp.float32)
    for sweep in range(ITERS):
        buf = sweep % 2
        last = sweep == ITERS - 1
        exchange(sweep, buf)
        if sweep == 0:
            wait_moves(1)
            wait_moves(2)
        total = coarse_pass(buf, last)
        if last:
            lax.fori_loop(1, n_gy, back_start, 0)
            own_back.start()
        total = total + fine_pass(buf)
        sums = jnp.where(row == sweep, jnp.sum(total, axis=0, keepdims=True), sums)

    def spread_sum(slots, axis, me, count, send_sems, recv_sems, between):
        def message(step, place_step):
            peer = lax.rem(me + step, count)
            return pltpu.make_async_remote_copy(
                slots.at[me],
                slots.at[lax.rem(me + place_step, count)],
                send_sems.at[step],
                recv_sems.at[step],
                device_id={axis: peer},
                device_id_type=MESH,
            )

        def start(step, carry):
            message(step, 0).start()
            return carry

        def wait(step, carry):
            message(step, count - step).wait()
            return carry

        lax.fori_loop(1, count, start, 0)
        between()
        lax.fori_loop(1, count, wait, 0)
        return lax.fori_loop(
            0, count, lambda i, acc: acc + slots[i], jnp.zeros((SUB, LANES), jnp.float32)
        )

    final = ITERS % 2
    weave_a = jnp.where(lane % 2 == 0, lane // 2, lane // 2 + LANES // 2)
    weave_b = jnp.where(lane % 2 == 0, lane // 2 + LANES // 2, lane // 2)

    def weave(i, carry):
        comp, block = i // blocks, i % blocks
        for parity in range(2):
            for half in range(halves):
                even = fine[final, comp, parity, 0, half, rows_of(block), :]
                odd = pltpu.roll(fine[final, comp, parity, 1, half, rows_of(block), :], LANES // 2, 1)
                at = pl.ds(block * 2 * SUB + parity, SUB, stride=2)
                raw_start[2 * half, comp, at, :] = jnp.take_along_axis(
                    jnp.where(half_lane, even, odd), weave_a, axis=1
                )
                raw_start[2 * half + 1, comp, at, :] = jnp.take_along_axis(
                    jnp.where(half_lane, odd, even), weave_b, axis=1
                )
        return carry

    stores = [
        pltpu.make_async_copy(
            raw_start.at[tile],
            fine_out.at[:, :, pl.ds(tile * LANES, LANES)],
            store_sem.at[tile],
        )
        for tile in range(tiles)
    ]

    def put_fine():
        lax.fori_loop(0, comps * blocks, weave, 0)
        for copy in stores:
            copy.start()

    norm_x[gx] = sums
    partial = spread_sum(norm_x, "gx", gx, n_gx, normx_send, normx_recv, put_fine)
    norm_y[gy] = partial
    whole = spread_sum(norm_y, "gy", gy, n_gy, normy_send, normy_recv, lambda: None)
    root = jnp.sqrt(jnp.sum(whole, axis=1, keepdims=True) / cells_total)
    norms_out[...] = jnp.broadcast_to(root, norms_out.shape)

    for copy in stores:
        copy.wait()
    own_back.wait()
    lax.fori_loop(1, n_gy, back_wait, 0)


def on_device(n_gx, n_gy, fine_start, fine_known, fine_mu, coarse_start, coarse_known, coarse_mu):
    comps, fine_rows, fine_cols = fine_start.shape
    rows, width = fine_rows // 2, fine_cols // 2
    halves = width // LANES
    tiles = 2 * halves
    padded = rows + 2 * SUB
    cells_total = 3.0 * (fine_mu.size + coarse_mu.size) * n_gx * n_gy
    f32 = jnp.float32
    dma = pltpu.SemaphoreType.DMA
    anywhere = pl.BlockSpec(memory_space=pl.ANY)
    fine_ghost, coarse_ghost, norms = pl.pallas_call(
        functools.partial(kernel, n_gx, n_gy, cells_total),
        out_shape=(
            jax.ShapeDtypeStruct(fine_start.shape, f32),
            jax.ShapeDtypeStruct(coarse_start.shape, f32),
            jax.ShapeDtypeStruct((SUB, LANES), f32),
        ),
        in_specs=[anywhere] * 6,
        out_specs=(anywhere, anywhere, pl.BlockSpec(memory_space=pltpu.VMEM)),
        scratch_shapes=[
            pltpu.VMEM((tiles, comps, fine_rows, LANES), f32),
            pltpu.VMEM((tiles, comps, fine_rows, LANES), f32),
            pltpu.VMEM((tiles, fine_rows, LANES), f32),
            pltpu.VMEM((2, comps, 2, 2, halves, padded, LANES), f32),
            pltpu.VMEM((comps, 2, 2, halves, rows, LANES), f32),
            pltpu.VMEM((2, 2, halves, rows, LANES), f32),
            pltpu.VMEM((2, 2, halves, rows, LANES), f32),
            pltpu.VMEM((comps, rows, width), f32),
            pltpu.VMEM((comps, rows, width), f32),
            pltpu.VMEM((rows, width), f32),
            pltpu.VMEM((2, comps, halves, padded, LANES), f32),
            pltpu.VMEM((comps, rows, width), f32),
            pltpu.VMEM((ITERS, 2, halves, 2 * SUB, LANES), f32),
            pltpu.VMEM((2, rows, LANES), f32),
            pltpu.VMEM((ITERS, 2, 2 * SUB, rows), f32),
            pltpu.VMEM((ITERS, 2, halves, 2 * SUB, LANES), f32),
            pltpu.VMEM((ITERS, 2, LANES, rows), f32),
            pltpu.VMEM((ITERS, 4, SUB, LANES), f32),
            pltpu.VMEM((padded, LANES), f32),
            pltpu.VMEM((padded, LANES), f32),
            pltpu.VMEM((n_gx, SUB, LANES), f32),
            pltpu.VMEM((n_gy, SUB, LANES), f32),
            dma((3, tiles)),
            dma((tiles,)),
            dma((3,)),
            dma((3, n_gy)),
            dma((3, n_gy)),
            dma((ITERS, 8)),
            dma((ITERS, 8)),
            dma((1,)),
            dma((n_gy,)),
            dma((n_gy,)),
            dma((n_gx,)),
            dma((n_gx,)),
            dma((n_gy,)),
            dma((n_gy,)),
        ],
        compiler_params=pltpu.CompilerParams(
            collective_id=0, has_side_effects=True, vmem_limit_bytes=48 * 1024 * 1024
        ),
    )(fine_start, fine_known, fine_mu, coarse_start, coarse_known, coarse_mu)
    return fine_ghost, coarse_ghost, norms[:ITERS, 0]


def solution(mesh):
    n_gx, n_gy = mesh.shape["gx"], mesh.shape["gy"]
    return jax.shard_map(
        functools.partial(on_device, n_gx, n_gy),
        mesh=mesh,
        in_specs=(
            P(None, "gx", "gy"),
            P(None, "gx", "gy"),
            P("gx", "gy"),
            P(None, ("gx", "gy"), None),
            P(None, ("gx", "gy"), None),
            P(("gx", "gy"), None),
        ),
        out_specs=(P(None, "gx", "gy"), P(None, ("gx", "gy"), None), P()),
        check_vma=False,
    )
```

```python
import functools

import jax
import jax.numpy as jnp
from jax import lax
from jax.experimental import pallas as pl
from jax.experimental.pallas import tpu as pltpu
from jax.sharding import PartitionSpec as P

ITERS = 3
LANES = 128
SUB = 8
UNROLL = 2
MESH = pl.DeviceIdType.MESH
DIRECTIONS = ((-1, 0), (1, 0), (0, -1), (0, 1), (-1, -1), (1, 1), (-1, 1), (1, -1))


def lane_index():
    return lax.broadcasted_iota(jnp.int32, (SUB, LANES), 1)


def roll_lanes(cells, shift):
    shift = shift % LANES
    return cells if shift == 0 else pltpu.roll(cells, shift, 1)


def from_left(halves, halo):
    first = lane_index() == 0
    rolled = [roll_lanes(cells, 1) for cells in halves]
    return [jnp.where(first, before, own) for before, own in zip([halo] + rolled[:-1], rolled)]


def from_right(halves, halo):
    last = lane_index() == LANES - 1
    rolled = [roll_lanes(cells, LANES - 1) for cells in halves]
    return [jnp.where(last, after, own) for own, after in zip(rolled, rolled[1:] + [halo])]


def kernel(
    n_gx,
    n_gy,
    cells_total,
    fine_start,
    fine_known,
    fine_mu,
    coarse_start,
    coarse_known,
    coarse_mu,
    fine_out,
    coarse_out,
    norms_out,
    raw_start,
    raw_known,
    raw_mu,
    fine_a,
    fine_b,
    known,
    diag,
    inverse,
    patch_start,
    patch_known,
    patch_mu,
    coarse_a,
    coarse_b,
    patch_out,
    row_send,
    col_send,
    col_out,
    row_recv,
    col_recv,
    corner_recv,
    left_halo,
    right_halo,
    norm_x,
    norm_y,
    load_sem,
    store_sem,
    own_sem,
    move_send,
    move_recv,
    halo_send,
    halo_recv,
    back_own,
    back_send,
    back_recv,
    normx_send,
    normx_recv,
    normy_send,
    normy_recv,
):
    gx = lax.axis_index("gx")
    gy = lax.axis_index("gy")
    fine, coarse = (fine_a, fine_b), (coarse_a, coarse_b)
    comps, rows, width = patch_start.shape
    halves = width // LANES
    blocks = rows // SUB
    own_rows = coarse_start.shape[1]
    lane = lane_index()

    loads = []
    for which, (source, target) in enumerate(
        ((fine_start, raw_start), (fine_mu, raw_mu), (fine_known, raw_known))
    ):
        for tile in range(2 * halves):
            at = pl.ds(tile * LANES, LANES)
            view = source.at[:, at] if len(source.shape) == 2 else source.at[:, :, at]
            loads.append(
                pltpu.make_async_copy(view, target.at[tile], load_sem.at[which, tile])
            )
    for copy in loads:
        copy.start()

    row_recv[...] = jnp.zeros_like(row_recv)
    col_recv[...] = jnp.zeros_like(col_recv)
    corner_recv[...] = jnp.zeros_like(corner_recv)
    col_send[...] = jnp.zeros_like(col_send)
    row_send[...] = jnp.zeros_like(row_send)

    barrier = pltpu.get_barrier_semaphore()

    def greet_gy(step, carry):
        pl.semaphore_signal(
            barrier, inc=1, device_id={"gy": lax.rem(gy + step, n_gy)}, device_id_type=MESH
        )
        return carry

    def greet_gx(step, carry):
        pl.semaphore_signal(
            barrier, inc=1, device_id={"gx": lax.rem(gx + step, n_gx)}, device_id_type=MESH
        )
        return carry

    lax.fori_loop(1, n_gy, greet_gy, 0)
    lax.fori_loop(1, n_gx, greet_gx, 0)

    def inside(direction):
        dx, dy = DIRECTIONS[direction]
        checks = []
        if dx:
            checks.append(gx > 0 if dx < 0 else gx < n_gx - 1)
        if dy:
            checks.append(gy > 0 if dy < 0 else gy < n_gy - 1)
        return functools.reduce(jnp.logical_and, checks)

    for direction in range(4, 8):
        dx, dy = DIRECTIONS[direction]

        @pl.when(inside(direction))
        def _():
            pl.semaphore_signal(
                barrier, inc=1, device_id={"gx": gx + dx, "gy": gy + dy}, device_id_type=MESH
            )

    sides_x = (gx > 0).astype(jnp.int32) + (gx < n_gx - 1).astype(jnp.int32)
    sides_y = (gy > 0).astype(jnp.int32) + (gy < n_gy - 1).astype(jnp.int32)
    pl.semaphore_wait(barrier, n_gy - 1 + n_gx - 1 + sides_x * sides_y)

    moved = ((coarse_start, patch_start), (coarse_known, patch_known), (coarse_mu, patch_mu))

    def move(which, owner, place, sem):
        source, target = moved[which]
        columns = pl.ds(pl.multiple_of(owner * width, LANES), width)
        lines = pl.ds(pl.multiple_of(place * own_rows, SUB), own_rows)
        if len(source.shape) == 2:
            return source.at[:, columns], target.at[lines, :]
        return source.at[:, :, columns], target.at[:, lines, :]

    def own_move(which):
        source, target = move(which, gy, gy, None)
        return pltpu.make_async_copy(source, target, own_sem.at[which])

    def peer_move(which, step):
        peer = lax.rem(gy + step, n_gy)
        source, target = move(which, peer, gy, None)
        return pltpu.make_async_remote_copy(
            source,
            target,
            move_send.at[which, step],
            move_recv.at[which, step],
            device_id={"gy": peer},
            device_id_type=MESH,
        )

    def wait_moves(which):
        own_move(which).wait()

        def body(step, carry):
            peer = lax.rem(gy + n_gy - step, n_gy)
            source, target = move(which, gy, peer, None)
            pltpu.make_async_remote_copy(
                source,
                target,
                move_send.at[which, step],
                move_recv.at[which, step],
                device_id={"gy": lax.rem(gy + step, n_gy)},
                device_id_type=MESH,
            ).wait()
            return carry

        lax.fori_loop(1, n_gy, body, 0)

    for which in range(3):

        def send_step(step, carry, which=which):
            peer_move(which, step).start()
            return carry

        lax.fori_loop(1, n_gy, send_step, 0)
        own_move(which).start()

    half_lane = lane < LANES // 2
    evens_first = jnp.where(half_lane, 2 * lane, 2 * lane - LANES + 1)
    odds_first = jnp.where(half_lane, 2 * lane + 1, 2 * lane - LANES)

    def split_columns(a, b):
        a = jnp.take_along_axis(a, evens_first, axis=1)
        b = jnp.take_along_axis(b, odds_first, axis=1)
        return (
            jnp.where(half_lane, a, b),
            pltpu.roll(jnp.where(half_lane, b, a), LANES // 2, 1),
        )

    def split_field(raw, put):
        def body(block, carry):
            out = []
            for comp in range(comps):
                for parity in range(2):
                    for half in range(halves):
                        at = pl.ds(block * 2 * SUB + parity, SUB, stride=2)
                        both = split_columns(
                            raw[2 * half, comp, at, :], raw[2 * half + 1, comp, at, :]
                        )
                        out.append((comp, parity, half, both))
            for comp, parity, half, both in out:
                put(comp, parity, 0, half, block, both[0])
                put(comp, parity, 1, half, block, both[1])
            return carry

        lax.fori_loop(0, blocks, body, 0)

    def rows_of(block, shift=0):
        if shift == 0:
            return pl.ds(pl.multiple_of(block * SUB + SUB, SUB), SUB)
        return pl.ds(block * SUB + SUB + shift, SUB)

    def plain(block):
        return pl.ds(pl.multiple_of(block * SUB, SUB), SUB)

    def put_start(comp, parity, side, half, block, cells):
        fine[0][comp, parity, side, half, rows_of(block), :] = cells

    def put_known(comp, parity, side, half, block, cells):
        known[comp, parity, side, half, plain(block), :] = cells

    def split_mu(block, carry):
        out = []
        for parity in range(2):
            for half in range(halves):
                at = pl.ds(block * 2 * SUB + parity, SUB, stride=2)
                both = split_columns(raw_mu[2 * half, at, :], raw_mu[2 * half + 1, at, :])
                for side in range(2):
                    total = both[side] + 1.0
                    out.append((parity, side, half, total, 1.0 / total))
        for parity, side, half, total, reciprocal in out:
            diag[parity, side, half, plain(block), :] = total
            inverse[parity, side, half, plain(block), :] = reciprocal
        return carry

    tiles = 2 * halves
    for copy in loads[:tiles]:
        copy.wait()
    split_field(raw_start, put_start)
    for copy in loads[tiles : 2 * tiles]:
        copy.wait()
    lax.fori_loop(0, blocks, split_mu, 0, unroll=2)
    for copy in loads[2 * tiles :]:
        copy.wait()
    split_field(raw_known, put_known)

    wait_moves(0)

    def place_start(block, carry):
        for comp in range(comps):
            for half in range(halves):
                coarse[0][comp, half, rows_of(block), :] = patch_start[
                    comp, plain(block), half * LANES : (half + 1) * LANES
                ]
        return carry

    lax.fori_loop(0, blocks, place_start, 0, unroll=4)

    def exchange(sweep, buf):
        for way, (parity, line) in enumerate(((0, SUB), (1, SUB + rows - 1))):
            for half in range(halves):
                for comp in range(comps):
                    for side in range(2):
                        at = 2 * comp + side
                        row_send[sweep, way, half, at : at + 1, :] = fine[buf][comp, parity, side, half, line : line + 1, :
                        ]
                    row_send[sweep, way, half, SUB + comp : SUB + comp + 1, :] = coarse[buf][comp, half, line : line + 1, :
                    ]

        def message(direction):
            dx, dy = DIRECTIONS[direction]
            way = direction % 2
            if direction < 2:
                source, target = row_send.at[sweep, way], row_recv.at[sweep, 1 - way]
            elif direction < 4:
                source = col_out.at[sweep, way]
                target = col_recv.at[sweep, 1 - way, pl.ds(0, 2 * SUB), :]
            else:
                half = 0 if dy < 0 else halves - 1
                source = row_send.at[sweep, 0 if dx < 0 else 1, half, pl.ds(SUB, SUB), :]
                target = corner_recv.at[sweep, (direction ^ 1) - 4]
            return pltpu.make_async_remote_copy(
                source,
                target,
                halo_send.at[sweep, direction],
                halo_recv.at[sweep, direction ^ 1],
                device_id={"gx": gx + dx, "gy": gy + dy},
                device_id_type=MESH,
            )

        for direction in (4, 5, 6, 7, 0, 1):

            @pl.when(inside(direction))
            def _():
                message(direction).start()

        def gather(block, carry):
            for way, (half, at, side) in enumerate(((0, 0, 0), (halves - 1, LANES - 1, 1))):
                cells = jnp.zeros((SUB, LANES), jnp.float32)
                for k in range(3 * comps):
                    if k < 2 * comps:
                        edge = fine[buf][k // 2, k % 2, side, half, rows_of(block), :]
                    else:
                        edge = coarse[buf][k - 2 * comps, half, rows_of(block), :]
                    cells = jnp.where(lane == k, roll_lanes(edge, k - at), cells)
                col_send[way, plain(block), :] = cells
            return carry

        lax.fori_loop(0, blocks, gather, 0, unroll=4)
        for way in range(2):
            turned = col_send[way, :, :].T
            col_turned = turned[: 2 * SUB]
            col_out[sweep, way, :, :] = col_turned

        for direction in (2, 3):

            @pl.when(inside(direction))
            def _():
                message(direction).start()

        for direction in range(8):

            @pl.when(inside(direction))
            def _():
                message(direction).wait_send()
                message(direction ^ 1).wait_recv()

        for half in range(halves):
            for comp in range(comps):
                for side in range(2):
                    at = 2 * comp + side
                    fine[buf][comp, 1, side, half, SUB - 1 : SUB, :] = row_recv[
                        sweep, 0, half, at : at + 1, :
                    ]
                    fine[buf][comp, 0, side, half, SUB + rows : SUB + rows + 1, :] = row_recv[
                        sweep, 1, half, at : at + 1, :
                    ]
                for way, line in enumerate((SUB - 1, SUB + rows)):
                    coarse[buf][comp, half, line : line + 1, :] = row_recv[
                        sweep, way, half, SUB + comp : SUB + comp + 1, :
                    ]
        left_halo[SUB : SUB + rows, :] = col_recv[sweep, 0].T
        right_halo[SUB : SUB + rows, :] = col_recv[sweep, 1].T
        for target, corners, at in ((left_halo, (0, 3), LANES - 1), (right_halo, (2, 1), 0)):
            for corner, line in zip(corners, (SUB - 1, SUB + rows)):
                block = corner_recv[sweep, corner]
                held = jnp.zeros((SUB, LANES), jnp.float32)
                for comp in range(comps):
                    k = 2 * comps + comp
                    held = jnp.where(
                        lane == k, roll_lanes(pltpu.roll(block, (SUB - comp) % SUB, 0)
                                              if comp else block, k - at), held
                    )
                target[line : line + 1, :] = held[0:1, :]

    def halo_pair(k, lines):
        left = roll_lanes(left_halo[lines, :], -k)
        right = roll_lanes(right_halo[lines, :], LANES - 1 - k)
        return left, right

    def coarse_pass(buf, last):
        def body(block, totals):
            totals = list(totals)
            lines = plain(block)
            out = []
            scales = [
                patch_mu[lines, half * LANES : (half + 1) * LANES] + 1.0 for half in range(halves)
            ]
            reciprocals = [1.0 / scale for scale in scales]
            for comp in range(comps):
                left, right = halo_pair(2 * comps + comp, rows_of(block))
                own = [coarse[buf][comp, half, rows_of(block), :] for half in range(halves)]
                lefts, rights = from_left(own, left), from_right(own, right)
                for half in range(halves):
                    columns = slice(half * LANES, (half + 1) * LANES)
                    near = (
                        coarse[buf][comp, half, rows_of(block, 1), :]
                        + coarse[buf][comp, half, rows_of(block, -1), :]
                        + rights[half]
                        + lefts[half]
                    )
                    below = (
                        fine[buf][comp, 0, 0, half, rows_of(block), :]
                        + fine[buf][comp, 1, 0, half, rows_of(block), :]
                        + fine[buf][comp, 0, 1, half, rows_of(block), :]
                        + fine[buf][comp, 1, 1, half, rows_of(block), :]
                    )
                    res = (
                        patch_known[comp, lines, columns]
                        + 0.25 * near
                        + 0.125 * below
                        - scales[half] * own[half]
                    )
                    totals[comp] = totals[comp] + res * res
                    out.append((comp, half, own[half] + res * reciprocals[half]))
            for comp, half, new in out:
                if last:
                    patch_out[comp, lines, half * LANES : (half + 1) * LANES] = new
                else:
                    coarse[1 - buf][comp, half, rows_of(block), :] = new
            return tuple(totals)

        zero = jnp.zeros((SUB, LANES), jnp.float32)
        return sum(lax.fori_loop(0, blocks, body, (zero,) * comps, unroll=UNROLL))

    def fine_pass(buf):
        def body(block, totals):
            totals = list(totals)
            out = []
            for comp in range(comps):
                k = 2 * comps + comp
                mid = [coarse[buf][comp, half, rows_of(block), :] for half in range(halves)]
                mid_left, mid_right = halo_pair(k, rows_of(block))
                for parity in range(2):
                    shift = 1 if parity else -1
                    far_left, far_right = halo_pair(k, rows_of(block, shift))
                    line = [
                        0.75 * mid[half]
                        + 0.25 * coarse[buf][comp, half, rows_of(block, shift), :]
                        for half in range(halves)
                    ]
                    line_left = from_left(line, 0.75 * mid_left + 0.25 * far_left)
                    line_right = from_right(line, 0.75 * mid_right + 0.25 * far_right)
                    fine_left, fine_right = halo_pair(2 * comp + parity, rows_of(block))
                    evens, odds = (
                        [fine[buf][comp, parity, side, half, rows_of(block), :] for half in range(halves)]
                        for side in range(2)
                    )
                    before, after = from_left(odds, fine_left), from_right(evens, fine_right)
                    for half in range(halves):
                        for side in range(2):
                            own = odds[half] if side else evens[half]
                            lateral = (
                                evens[half] + after[half] if side else odds[half] + before[half]
                            )
                            near = (
                                fine[buf][comp, 1 - parity, side, half, rows_of(block), :]
                                + fine[buf][comp, 1 - parity, side, half, rows_of(block, shift), :]
                                + lateral
                            )
                            spread = 0.75 * line[half] + 0.25 * (
                                line_right[half] if side else line_left[half]
                            )
                            res = (
                                known[comp, parity, side, half, plain(block), :]
                                + 0.25 * near
                                + 0.5 * spread
                                - diag[parity, side, half, plain(block), :] * own
                            )
                            totals[comp] = totals[comp] + res * res
                            new = own + res * inverse[parity, side, half, plain(block), :]
                            out.append((comp, parity, side, half, new))
            for comp, parity, side, half, new in out:
                fine[1 - buf][comp, parity, side, half, rows_of(block), :] = new
            return tuple(totals)

        zero = jnp.zeros((SUB, LANES), jnp.float32)
        return sum(lax.fori_loop(0, blocks, body, (zero,) * comps))

    def back_place(owner, place):
        return (
            patch_out.at[:, pl.ds(pl.multiple_of(owner * own_rows, SUB), own_rows), :],
            coarse_out.at[:, :, pl.ds(pl.multiple_of(place * width, LANES), width)],
        )

    def back_move(step, place_step):
        peer = lax.rem(gy + step, n_gy)
        source, _ = back_place(peer, gy)
        _, target = back_place(peer, lax.rem(gy + place_step, n_gy))
        return pltpu.make_async_remote_copy(
            source,
            target,
            back_send.at[step],
            back_recv.at[step],
            device_id={"gy": peer},
            device_id_type=MESH,
        )

    def back_start(step, carry):
        back_move(step, 0).start()
        return carry

    def back_wait(step, carry):
        back_move(step, n_gy - step).wait()
        return carry

    own_back = pltpu.make_async_copy(*back_place(gy, gy), back_own.at[0])
    row = lax.broadcasted_iota(jnp.int32, (SUB, LANES), 0)
    sums = jnp.zeros((SUB, LANES), jnp.float32)
    for sweep in range(ITERS):
        buf = sweep % 2
        last = sweep == ITERS - 1
        exchange(sweep, buf)
        if sweep == 0:
            wait_moves(1)
            wait_moves(2)
        total = coarse_pass(buf, last)
        if last:
            lax.fori_loop(1, n_gy, back_start, 0)
            own_back.start()
        total = total + fine_pass(buf)
        sums = jnp.where(row == sweep, jnp.sum(total, axis=0, keepdims=True), sums)

    def spread_sum(slots, axis, me, count, send_sems, recv_sems, between):
        def message(step, place_step):
            peer = lax.rem(me + step, count)
            return pltpu.make_async_remote_copy(
                slots.at[me],
                slots.at[lax.rem(me + place_step, count)],
                send_sems.at[step],
                recv_sems.at[step],
                device_id={axis: peer},
                device_id_type=MESH,
            )

        def start(step, carry):
            message(step, 0).start()
            return carry

        def wait(step, carry):
            message(step, count - step).wait()
            return carry

        lax.fori_loop(1, count, start, 0)
        between()
        lax.fori_loop(1, count, wait, 0)
        return lax.fori_loop(
            0, count, lambda i, acc: acc + slots[i], jnp.zeros((SUB, LANES), jnp.float32)
        )

    final = ITERS % 2
    weave_a = jnp.where(lane % 2 == 0, lane // 2, lane // 2 + LANES // 2)
    weave_b = jnp.where(lane % 2 == 0, lane // 2 + LANES // 2, lane // 2)

    def weave(block, carry):
        out = []
        for comp in range(comps):
            for parity in range(2):
                for half in range(halves):
                    even = fine[final][comp, parity, 0, half, rows_of(block), :]
                    odd = fine[final][comp, parity, 1, half, rows_of(block), :]
                    odd = pltpu.roll(odd, LANES // 2, 1)
                    at = pl.ds(block * 2 * SUB + parity, SUB, stride=2)
                    a = jnp.take_along_axis(jnp.where(half_lane, even, odd), weave_a, axis=1)
                    b = jnp.take_along_axis(jnp.where(half_lane, odd, even), weave_b, axis=1)
                    out.append((2 * half, comp, at, a))
                    out.append((2 * half + 1, comp, at, b))
        for tile, comp, at, cells in out:
            raw_start[tile, comp, at, :] = cells
        return carry

    stores = [
        pltpu.make_async_copy(
            raw_start.at[tile],
            fine_out.at[:, :, pl.ds(tile * LANES, LANES)],
            store_sem.at[tile],
        )
        for tile in range(tiles)
    ]

    def put_fine():
        lax.fori_loop(0, blocks, weave, 0)
        for copy in stores:
            copy.start()

    norm_x[gx] = sums
    partial = spread_sum(norm_x, "gx", gx, n_gx, normx_send, normx_recv, put_fine)
    norm_y[gy] = partial
    whole = spread_sum(norm_y, "gy", gy, n_gy, normy_send, normy_recv, lambda: None)
    root = jnp.sqrt(jnp.sum(whole, axis=1, keepdims=True) / cells_total)
    norms_out[...] = jnp.broadcast_to(root, norms_out.shape)

    for copy in stores:
        copy.wait()
    own_back.wait()
    lax.fori_loop(1, n_gy, back_wait, 0)


def on_device(n_gx, n_gy, fine_start, fine_known, fine_mu, coarse_start, coarse_known, coarse_mu):
    comps, fine_rows, fine_cols = fine_start.shape
    rows, width = fine_rows // 2, fine_cols // 2
    halves = width // LANES
    tiles = 2 * halves
    padded = rows + 2 * SUB
    cells_total = 3.0 * (fine_mu.size + coarse_mu.size) * n_gx * n_gy
    f32 = jnp.float32
    dma = pltpu.SemaphoreType.DMA
    anywhere = pl.BlockSpec(memory_space=pl.ANY)
    fine_ghost, coarse_ghost, norms = pl.pallas_call(
        functools.partial(kernel, n_gx, n_gy, cells_total),
        out_shape=(
            jax.ShapeDtypeStruct(fine_start.shape, f32),
            jax.ShapeDtypeStruct(coarse_start.shape, f32),
            jax.ShapeDtypeStruct((SUB, LANES), f32),
        ),
        in_specs=[anywhere] * 6,
        out_specs=(anywhere, anywhere, pl.BlockSpec(memory_space=pltpu.VMEM)),
        scratch_shapes=[
            pltpu.VMEM((tiles, comps, fine_rows, LANES), f32),
            pltpu.VMEM((tiles, comps, fine_rows, LANES), f32),
            pltpu.VMEM((tiles, fine_rows, LANES), f32),
            pltpu.VMEM((comps, 2, 2, halves, padded, LANES), f32),
            pltpu.VMEM((comps, 2, 2, halves, padded, LANES), f32),
            pltpu.VMEM((comps, 2, 2, halves, rows, LANES), f32),
            pltpu.VMEM((2, 2, halves, rows, LANES), f32),
            pltpu.VMEM((2, 2, halves, rows, LANES), f32),
            pltpu.VMEM((comps, rows, width), f32),
            pltpu.VMEM((comps, rows, width), f32),
            pltpu.VMEM((rows, width), f32),
            pltpu.VMEM((comps, halves, padded, LANES), f32),
            pltpu.VMEM((comps, halves, padded, LANES), f32),
            pltpu.VMEM((comps, rows, width), f32),
            pltpu.VMEM((ITERS, 2, halves, 2 * SUB, LANES), f32),
            pltpu.VMEM((2, rows, LANES), f32),
            pltpu.VMEM((ITERS, 2, 2 * SUB, rows), f32),
            pltpu.VMEM((ITERS, 2, halves, 2 * SUB, LANES), f32),
            pltpu.VMEM((ITERS, 2, LANES, rows), f32),
            pltpu.VMEM((ITERS, 4, SUB, LANES), f32),
            pltpu.VMEM((padded, LANES), f32),
            pltpu.VMEM((padded, LANES), f32),
            pltpu.VMEM((n_gx, SUB, LANES), f32),
            pltpu.VMEM((n_gy, SUB, LANES), f32),
            dma((3, tiles)),
            dma((tiles,)),
            dma((3,)),
            dma((3, n_gy)),
            dma((3, n_gy)),
            dma((ITERS, 8)),
            dma((ITERS, 8)),
            dma((1,)),
            dma((n_gy,)),
            dma((n_gy,)),
            dma((n_gx,)),
            dma((n_gx,)),
            dma((n_gy,)),
            dma((n_gy,)),
        ],
        compiler_params=pltpu.CompilerParams(
            collective_id=0, has_side_effects=True, vmem_limit_bytes=48 * 1024 * 1024
        ),
    )(fine_start, fine_known, fine_mu, coarse_start, coarse_known, coarse_mu)
    return fine_ghost, coarse_ghost, norms[:ITERS, 0]


def solution(mesh):
    n_gx, n_gy = mesh.shape["gx"], mesh.shape["gy"]
    return jax.shard_map(
        functools.partial(on_device, n_gx, n_gy),
        mesh=mesh,
        in_specs=(
            P(None, "gx", "gy"),
            P(None, "gx", "gy"),
            P("gx", "gy"),
            P(None, ("gx", "gy"), None),
            P(None, ("gx", "gy"), None),
            P(("gx", "gy"), None),
        ),
        out_specs=(P(None, "gx", "gy"), P(None, ("gx", "gy"), None), P()),
        check_vma=False,
    )
```

```python
import functools

import jax
import jax.numpy as jnp
from jax import lax
from jax.experimental import pallas as pl
from jax.experimental.pallas import tpu as pltpu
from jax.sharding import PartitionSpec as P

ITERS = 3
LANES = 128
SUB = 8
UNROLL = 2
MESH = pl.DeviceIdType.MESH
DIRECTIONS = ((-1, 0), (1, 0), (0, -1), (0, 1), (-1, -1), (1, 1), (-1, 1), (1, -1))


def lane_index():
    return lax.broadcasted_iota(jnp.int32, (SUB, LANES), 1)


def roll_lanes(cells, shift):
    shift = shift % LANES
    return cells if shift == 0 else pltpu.roll(cells, shift, 1)


def from_left(halves, halo):
    first = lane_index() == 0
    rolled = [roll_lanes(cells, 1) for cells in halves]
    return [jnp.where(first, before, own) for before, own in zip([halo] + rolled[:-1], rolled)]


def from_right(halves, halo):
    last = lane_index() == LANES - 1
    rolled = [roll_lanes(cells, LANES - 1) for cells in halves]
    return [jnp.where(last, after, own) for own, after in zip(rolled, rolled[1:] + [halo])]


def kernel(
    n_gx,
    n_gy,
    cells_total,
    fine_start,
    fine_known,
    fine_mu,
    coarse_start,
    coarse_known,
    coarse_mu,
    fine_out,
    coarse_out,
    norms_out,
    raw_start,
    raw_known,
    raw_mu,
    fine_a,
    fine_b,
    known,
    diag,
    inverse,
    patch_start,
    patch_known,
    patch_mu,
    coarse_a,
    coarse_b,
    patch_out,
    fine_row_send,
    fine_row_recv,
    fine_col_send,
    fine_col_recv,
    row_send,
    row_recv,
    col_send,
    col_recv,
    corner_recv,
    packed,
    fine_halo,
    coarse_halo,
    norm_x,
    norm_y,
    load_sem,
    store_sem,
    own_sem,
    move_send,
    move_recv,
    fine_send,
    fine_recv,
    halo_send,
    halo_recv,
    back_own,
    back_send,
    back_recv,
    normx_send,
    normx_recv,
    normy_send,
    normy_recv,
):
    gx = lax.axis_index("gx")
    gy = lax.axis_index("gy")
    fine, coarse = (fine_a, fine_b), (coarse_a, coarse_b)
    comps, rows, width = patch_start.shape
    halves = width // LANES
    blocks = rows // SUB
    own_rows = coarse_start.shape[1]
    lane = lane_index()

    loads = []
    for which, (source, target) in enumerate(
        ((fine_start, raw_start), (fine_mu, raw_mu), (fine_known, raw_known))
    ):
        for tile in range(2 * halves):
            at = pl.ds(tile * LANES, LANES)
            view = source.at[:, at] if len(source.shape) == 2 else source.at[:, :, at]
            loads.append(
                pltpu.make_async_copy(view, target.at[tile], load_sem.at[which, tile])
            )
    for copy in loads:
        copy.start()

    for ref in (fine_row_recv, fine_col_recv, row_recv, col_recv, corner_recv, row_send, fine_row_send):
        ref[...] = jnp.zeros_like(ref)

    barrier = pltpu.get_barrier_semaphore()

    def greet_gy(step, carry):
        pl.semaphore_signal(
            barrier, inc=1, device_id={"gy": lax.rem(gy + step, n_gy)}, device_id_type=MESH
        )
        return carry

    def greet_gx(step, carry):
        pl.semaphore_signal(
            barrier, inc=1, device_id={"gx": lax.rem(gx + step, n_gx)}, device_id_type=MESH
        )
        return carry

    lax.fori_loop(1, n_gy, greet_gy, 0)
    lax.fori_loop(1, n_gx, greet_gx, 0)

    def inside(direction):
        dx, dy = DIRECTIONS[direction]
        checks = []
        if dx:
            checks.append(gx > 0 if dx < 0 else gx < n_gx - 1)
        if dy:
            checks.append(gy > 0 if dy < 0 else gy < n_gy - 1)
        return functools.reduce(jnp.logical_and, checks)

    for direction in range(4, 8):
        dx, dy = DIRECTIONS[direction]

        @pl.when(inside(direction))
        def _():
            pl.semaphore_signal(
                barrier, inc=1, device_id={"gx": gx + dx, "gy": gy + dy}, device_id_type=MESH
            )

    sides_x = (gx > 0).astype(jnp.int32) + (gx < n_gx - 1).astype(jnp.int32)
    sides_y = (gy > 0).astype(jnp.int32) + (gy < n_gy - 1).astype(jnp.int32)
    pl.semaphore_wait(barrier, n_gy - 1 + n_gx - 1 + sides_x * sides_y)

    moved = ((coarse_start, patch_start), (coarse_known, patch_known), (coarse_mu, patch_mu))

    def move(which, owner, place, sem):
        source, target = moved[which]
        columns = pl.ds(pl.multiple_of(owner * width, LANES), width)
        lines = pl.ds(pl.multiple_of(place * own_rows, SUB), own_rows)
        if len(source.shape) == 2:
            return source.at[:, columns], target.at[lines, :]
        return source.at[:, :, columns], target.at[:, lines, :]

    def own_move(which):
        source, target = move(which, gy, gy, None)
        return pltpu.make_async_copy(source, target, own_sem.at[which])

    def peer_move(which, step):
        peer = lax.rem(gy + step, n_gy)
        source, target = move(which, peer, gy, None)
        return pltpu.make_async_remote_copy(
            source,
            target,
            move_send.at[which, step],
            move_recv.at[which, step],
            device_id={"gy": peer},
            device_id_type=MESH,
        )

    def wait_moves(which):
        own_move(which).wait()

        def body(step, carry):
            peer = lax.rem(gy + n_gy - step, n_gy)
            source, target = move(which, gy, peer, None)
            pltpu.make_async_remote_copy(
                source,
                target,
                move_send.at[which, step],
                move_recv.at[which, step],
                device_id={"gy": lax.rem(gy + step, n_gy)},
                device_id_type=MESH,
            ).wait()
            return carry

        lax.fori_loop(1, n_gy, body, 0)

    def send_moves(which):
        def body(step, carry):
            peer_move(which, step).start()
            return carry

        lax.fori_loop(1, n_gy, body, 0)
        own_move(which).start()

    send_moves(0)

    half_lane = lane < LANES // 2
    evens_first = jnp.where(half_lane, 2 * lane, 2 * lane - LANES + 1)
    odds_first = jnp.where(half_lane, 2 * lane + 1, 2 * lane - LANES)

    def split_columns(a, b):
        a = jnp.take_along_axis(a, evens_first, axis=1)
        b = jnp.take_along_axis(b, odds_first, axis=1)
        return (
            jnp.where(half_lane, a, b),
            pltpu.roll(jnp.where(half_lane, b, a), LANES // 2, 1),
        )

    def split_field(raw, put):
        def body(block, carry):
            out = []
            for comp in range(comps):
                for parity in range(2):
                    for half in range(halves):
                        at = pl.ds(block * 2 * SUB + parity, SUB, stride=2)
                        both = split_columns(
                            raw[2 * half, comp, at, :], raw[2 * half + 1, comp, at, :]
                        )
                        out.append((comp, parity, half, both))
            for comp, parity, half, both in out:
                put(comp, parity, 0, half, block, both[0])
                put(comp, parity, 1, half, block, both[1])
            return carry

        lax.fori_loop(0, blocks, body, 0)

    def rows_of(block, shift=0):
        if shift == 0:
            return pl.ds(pl.multiple_of(block * SUB + SUB, SUB), SUB)
        return pl.ds(block * SUB + SUB + shift, SUB)

    def plain(block):
        return pl.ds(pl.multiple_of(block * SUB, SUB), SUB)

    def put_start(comp, parity, side, half, block, cells):
        fine[0][comp, parity, side, half, rows_of(block), :] = cells

    def put_known(comp, parity, side, half, block, cells):
        known[comp, parity, side, half, plain(block), :] = cells

    def split_mu(block, carry):
        out = []
        for parity in range(2):
            for half in range(halves):
                at = pl.ds(block * 2 * SUB + parity, SUB, stride=2)
                both = split_columns(raw_mu[2 * half, at, :], raw_mu[2 * half + 1, at, :])
                for side in range(2):
                    total = both[side] + 1.0
                    out.append((parity, side, half, total, 1.0 / total))
        for parity, side, half, total, reciprocal in out:
            diag[parity, side, half, plain(block), :] = total
            inverse[parity, side, half, plain(block), :] = reciprocal
        return carry

    def place_start(block, carry):
        for comp in range(comps):
            for half in range(halves):
                coarse[0][comp, half, rows_of(block), :] = patch_start[
                    comp, plain(block), half * LANES : (half + 1) * LANES
                ]
        return carry

    def pack(edges, target):
        def body(block, carry):
            out = []
            for way, at in ((0, 0), (1, LANES - 1)):
                for k, edge in enumerate(edges(way, block)):
                    out.append((SUB * way + k, roll_lanes(edge, SUB * way + k - at)))
            cells = jnp.zeros((SUB, LANES), jnp.float32)
            for k, edge in out:
                cells = jnp.where(lane == k, edge, cells)
            packed[plain(block), :] = cells
            return carry

        lax.fori_loop(0, blocks, body, 0, unroll=4)
        target[...] = packed[...].T[: 2 * SUB]

    def message(rows_out, rows_in, cols_out, cols_in, sends, recvs, sweep, direction):
        dx, dy = DIRECTIONS[direction]
        way = direction % 2
        if direction < 2:
            source, target = rows_out.at[sweep, way], rows_in.at[sweep, 1 - way]
        elif direction < 4:
            source = cols_out.at[sweep, pl.ds(SUB * way, SUB), :]
            target = cols_in.at[sweep, pl.ds(SUB * (1 - way), SUB), :]
        else:
            half = 0 if dy < 0 else halves - 1
            source = rows_out.at[sweep, 0 if dx < 0 else 1, half]
            target = corner_recv.at[sweep, (direction ^ 1) - 4]
        return pltpu.make_async_remote_copy(
            source,
            target,
            sends.at[sweep, direction],
            recvs.at[sweep, direction ^ 1],
            device_id={"gx": gx + dx, "gy": gy + dy},
            device_id_type=MESH,
        )

    fine_message = functools.partial(
        message, fine_row_send, fine_row_recv, fine_col_send, fine_col_recv, fine_send, fine_recv
    )
    coarse_message = functools.partial(
        message, row_send, row_recv, col_send, col_recv, halo_send, halo_recv
    )

    def start_all(of, sweep, directions):
        for direction in directions:

            @pl.when(inside(direction))
            def _():
                of(sweep, direction).start()

    def wait_all(of, sweep, directions):
        for direction in directions:

            @pl.when(inside(direction))
            def _():
                of(sweep, direction).wait_send()
                of(sweep, direction ^ 1).wait_recv()

    def send_fine(sweep):
        buf = sweep % 2
        for way, line in enumerate((SUB, SUB + rows - 1)):
            for half in range(halves):
                for comp in range(comps):
                    for side in range(2):
                        at = 2 * comp + side
                        fine_row_send[sweep, way, half, at : at + 1, :] = fine[buf][
                            comp, way, side, half, line : line + 1, :
                        ]
        start_all(fine_message, sweep, (0, 1))

        def edges(way, block):
            half = way * (halves - 1)
            return [
                fine[buf][k // 2, k % 2, way, half, rows_of(block), :] for k in range(2 * comps)
            ]

        pack(edges, fine_col_send.at[sweep])
        start_all(fine_message, sweep, (2, 3))

    def take_fine(sweep):
        buf = sweep % 2
        wait_all(fine_message, sweep, range(4))
        for half in range(halves):
            for comp in range(comps):
                for side in range(2):
                    at = 2 * comp + side
                    fine[buf][comp, 1, side, half, SUB - 1 : SUB, :] = fine_row_recv[
                        sweep, 0, half, at : at + 1, :
                    ]
                    fine[buf][comp, 0, side, half, SUB + rows : SUB + rows + 1, :] = (
                        fine_row_recv[sweep, 1, half, at : at + 1, :]
                    )
        fine_halo[SUB : SUB + rows, :] = fine_col_recv[sweep].T

    def send_coarse(sweep):
        buf = sweep % 2
        for way, line in enumerate((SUB, SUB + rows - 1)):
            for half in range(halves):
                for comp in range(comps):
                    row_send[sweep, way, half, comp : comp + 1, :] = coarse[buf][
                        comp, half, line : line + 1, :
                    ]
        start_all(coarse_message, sweep, (4, 5, 6, 7, 0, 1))

        def edges(way, block):
            half = way * (halves - 1)
            return [coarse[buf][k, half, rows_of(block), :] for k in range(comps)]

        pack(edges, col_send.at[sweep])
        start_all(coarse_message, sweep, (2, 3))

    def take_coarse(sweep):
        buf = sweep % 2
        wait_all(coarse_message, sweep, range(8))
        for half in range(halves):
            for comp in range(comps):
                for way, line in enumerate((SUB - 1, SUB + rows)):
                    coarse[buf][comp, half, line : line + 1, :] = row_recv[
                        sweep, way, half, comp : comp + 1, :
                    ]
        coarse_halo[SUB : SUB + rows, :] = col_recv[sweep].T
        corner_lanes = ((0, 2), (3, 1))
        for corners, line in zip(corner_lanes, (SUB - 1, SUB + rows)):
            held = jnp.zeros((SUB, LANES), jnp.float32)
            for way, corner in enumerate(corners):
                block = corner_recv[sweep, corner]
                for comp in range(comps):
                    k = SUB * way + comp
                    lifted = pltpu.roll(block, SUB - comp, 0) if comp else block
                    moved = roll_lanes(lifted, k - (0 if way else LANES - 1))
                    held = jnp.where(lane == k, moved, held)
            coarse_halo[line : line + 1, :] = held[0:1, :]

    def halo_pair(halo, k, lines):
        cells = halo[lines, :]
        return roll_lanes(cells, -k), roll_lanes(cells, LANES - 1 - SUB - k)

    def coarse_pass(buf, last):
        def body(block, totals):
            totals = list(totals)
            lines = plain(block)
            out = []
            scales = [
                patch_mu[lines, half * LANES : (half + 1) * LANES] + 1.0 for half in range(halves)
            ]
            reciprocals = [1.0 / scale for scale in scales]
            for comp in range(comps):
                left, right = halo_pair(coarse_halo, comp, rows_of(block))
                own = [coarse[buf][comp, half, rows_of(block), :] for half in range(halves)]
                lefts, rights = from_left(own, left), from_right(own, right)
                for half in range(halves):
                    columns = slice(half * LANES, (half + 1) * LANES)
                    near = (
                        coarse[buf][comp, half, rows_of(block, 1), :]
                        + coarse[buf][comp, half, rows_of(block, -1), :]
                        + rights[half]
                        + lefts[half]
                    )
                    below = (
                        fine[buf][comp, 0, 0, half, rows_of(block), :]
                        + fine[buf][comp, 1, 0, half, rows_of(block), :]
                        + fine[buf][comp, 0, 1, half, rows_of(block), :]
                        + fine[buf][comp, 1, 1, half, rows_of(block), :]
                    )
                    res = (
                        patch_known[comp, lines, columns]
                        + 0.25 * near
                        + 0.125 * below
                        - scales[half] * own[half]
                    )
                    totals[comp] = totals[comp] + res * res
                    out.append((comp, half, own[half] + res * reciprocals[half]))
            for comp, half, new in out:
                if last:
                    patch_out[comp, lines, half * LANES : (half + 1) * LANES] = new
                else:
                    coarse[1 - buf][comp, half, rows_of(block), :] = new
            return tuple(totals)

        zero = jnp.zeros((SUB, LANES), jnp.float32)
        return sum(lax.fori_loop(0, blocks, body, (zero,) * comps, unroll=UNROLL))

    def fine_pass(buf):
        def body(block, totals):
            totals = list(totals)
            out = []
            for comp in range(comps):
                mid = [coarse[buf][comp, half, rows_of(block), :] for half in range(halves)]
                mid_left, mid_right = halo_pair(coarse_halo, comp, rows_of(block))
                for parity in range(2):
                    shift = 1 if parity else -1
                    far_left, far_right = halo_pair(coarse_halo, comp, rows_of(block, shift))
                    line = [
                        0.75 * mid[half]
                        + 0.25 * coarse[buf][comp, half, rows_of(block, shift), :]
                        for half in range(halves)
                    ]
                    line_left = from_left(line, 0.75 * mid_left + 0.25 * far_left)
                    line_right = from_right(line, 0.75 * mid_right + 0.25 * far_right)
                    fine_left, fine_right = halo_pair(fine_halo, 2 * comp + parity, rows_of(block))
                    evens, odds = (
                        [fine[buf][comp, parity, side, half, rows_of(block), :] for half in range(halves)]
                        for side in range(2)
                    )
                    before, after = from_left(odds, fine_left), from_right(evens, fine_right)
                    for half in range(halves):
                        for side in range(2):
                            own = odds[half] if side else evens[half]
                            lateral = (
                                evens[half] + after[half] if side else odds[half] + before[half]
                            )
                            near = (
                                fine[buf][comp, 1 - parity, side, half, rows_of(block), :]
                                + fine[buf][comp, 1 - parity, side, half, rows_of(block, shift), :]
                                + lateral
                            )
                            spread = 0.75 * line[half] + 0.25 * (
                                line_right[half] if side else line_left[half]
                            )
                            res = (
                                known[comp, parity, side, half, plain(block), :]
                                + 0.25 * near
                                + 0.5 * spread
                                - diag[parity, side, half, plain(block), :] * own
                            )
                            totals[comp] = totals[comp] + res * res
                            new = own + res * inverse[parity, side, half, plain(block), :]
                            out.append((comp, parity, side, half, new))
            for comp, parity, side, half, new in out:
                fine[1 - buf][comp, parity, side, half, rows_of(block), :] = new
            return tuple(totals)

        zero = jnp.zeros((SUB, LANES), jnp.float32)
        return sum(lax.fori_loop(0, blocks, body, (zero,) * comps))

    def back_place(owner, place):
        return (
            patch_out.at[:, pl.ds(pl.multiple_of(owner * own_rows, SUB), own_rows), :],
            coarse_out.at[:, :, pl.ds(pl.multiple_of(place * width, LANES), width)],
        )

    def back_move(step, place_step):
        peer = lax.rem(gy + step, n_gy)
        source, _ = back_place(peer, gy)
        _, target = back_place(peer, lax.rem(gy + place_step, n_gy))
        return pltpu.make_async_remote_copy(
            source,
            target,
            back_send.at[step],
            back_recv.at[step],
            device_id={"gy": peer},
            device_id_type=MESH,
        )

    def back_start(step, carry):
        back_move(step, 0).start()
        return carry

    def back_wait(step, carry):
        back_move(step, n_gy - step).wait()
        return carry

    own_back = pltpu.make_async_copy(*back_place(gy, gy), back_own.at[0])
    row = lax.broadcasted_iota(jnp.int32, (SUB, LANES), 0)
    totals = [None] * ITERS
    tiles = 2 * halves
    for copy in loads[:tiles]:
        copy.wait()
    split_field(raw_start, put_start)
    send_fine(0)
    send_moves(2)
    for copy in loads[tiles : 2 * tiles]:
        copy.wait()
    lax.fori_loop(0, blocks, split_mu, 0, unroll=2)
    for copy in loads[2 * tiles :]:
        copy.wait()
    split_field(raw_known, put_known)
    wait_moves(0)
    lax.fori_loop(0, blocks, place_start, 0, unroll=4)
    send_coarse(0)
    send_moves(1)
    take_fine(0)
    take_coarse(0)

    totals[0] = fine_pass(0)
    send_fine(1)
    wait_moves(2)
    wait_moves(1)
    totals[0] = totals[0] + coarse_pass(0, False)
    for sweep in range(1, ITERS):
        buf = sweep % 2
        last = sweep == ITERS - 1
        if sweep == 1:
            send_coarse(1)
        take_coarse(sweep)
        totals[sweep] = coarse_pass(buf, last)
        if last:
            lax.fori_loop(1, n_gy, back_start, 0)
            own_back.start()
        else:
            send_coarse(sweep + 1)
        take_fine(sweep)
        totals[sweep] = totals[sweep] + fine_pass(buf)
        if not last:
            send_fine(sweep + 1)
    sums = jnp.zeros((SUB, LANES), jnp.float32)
    for sweep in range(ITERS):
        sums = jnp.where(row == sweep, jnp.sum(totals[sweep], axis=0, keepdims=True), sums)

    def spread_sum(slots, axis, me, count, send_sems, recv_sems, between):
        def message(step, place_step):
            peer = lax.rem(me + step, count)
            return pltpu.make_async_remote_copy(
                slots.at[me],
                slots.at[lax.rem(me + place_step, count)],
                send_sems.at[step],
                recv_sems.at[step],
                device_id={axis: peer},
                device_id_type=MESH,
            )

        def start(step, carry):
            message(step, 0).start()
            return carry

        def wait(step, carry):
            message(step, count - step).wait()
            return carry

        lax.fori_loop(1, count, start, 0)
        between()
        lax.fori_loop(1, count, wait, 0)
        return lax.fori_loop(
            0, count, lambda i, acc: acc + slots[i], jnp.zeros((SUB, LANES), jnp.float32)
        )

    final = ITERS % 2
    weave_a = jnp.where(lane % 2 == 0, lane // 2, lane // 2 + LANES // 2)
    weave_b = jnp.where(lane % 2 == 0, lane // 2 + LANES // 2, lane // 2)

    def weave(block, carry):
        out = []
        for comp in range(comps):
            for parity in range(2):
                for half in range(halves):
                    even = fine[final][comp, parity, 0, half, rows_of(block), :]
                    odd = fine[final][comp, parity, 1, half, rows_of(block), :]
                    odd = pltpu.roll(odd, LANES // 2, 1)
                    at = pl.ds(block * 2 * SUB + parity, SUB, stride=2)
                    a = jnp.take_along_axis(jnp.where(half_lane, even, odd), weave_a, axis=1)
                    b = jnp.take_along_axis(jnp.where(half_lane, odd, even), weave_b, axis=1)
                    out.append((2 * half, comp, at, a))
                    out.append((2 * half + 1, comp, at, b))
        for tile, comp, at, cells in out:
            raw_start[tile, comp, at, :] = cells
        return carry

    stores = [
        pltpu.make_async_copy(
            raw_start.at[tile],
            fine_out.at[:, :, pl.ds(tile * LANES, LANES)],
            store_sem.at[tile],
        )
        for tile in range(tiles)
    ]

    def put_fine():
        lax.fori_loop(0, blocks, weave, 0)
        for copy in stores:
            copy.start()

    norm_x[gx] = sums
    partial = spread_sum(norm_x, "gx", gx, n_gx, normx_send, normx_recv, put_fine)
    norm_y[gy] = partial
    whole = spread_sum(norm_y, "gy", gy, n_gy, normy_send, normy_recv, lambda: None)
    root = jnp.sqrt(jnp.sum(whole, axis=1, keepdims=True) / cells_total)
    norms_out[...] = jnp.broadcast_to(root, norms_out.shape)

    for copy in stores:
        copy.wait()
    own_back.wait()
    lax.fori_loop(1, n_gy, back_wait, 0)


def on_device(n_gx, n_gy, fine_start, fine_known, fine_mu, coarse_start, coarse_known, coarse_mu):
    comps, fine_rows, fine_cols = fine_start.shape
    rows, width = fine_rows // 2, fine_cols // 2
    halves = width // LANES
    tiles = 2 * halves
    padded = rows + 2 * SUB
    cells_total = 3.0 * (fine_mu.size + coarse_mu.size) * n_gx * n_gy
    f32 = jnp.float32
    dma = pltpu.SemaphoreType.DMA
    anywhere = pl.BlockSpec(memory_space=pl.ANY)
    fine_ghost, coarse_ghost, norms = pl.pallas_call(
        functools.partial(kernel, n_gx, n_gy, cells_total),
        out_shape=(
            jax.ShapeDtypeStruct(fine_start.shape, f32),
            jax.ShapeDtypeStruct(coarse_start.shape, f32),
            jax.ShapeDtypeStruct((SUB, LANES), f32),
        ),
        in_specs=[pl.BlockSpec(memory_space=pltpu.HBM)] * 6,
        out_specs=(anywhere, anywhere, pl.BlockSpec(memory_space=pltpu.VMEM)),
        scratch_shapes=[
            pltpu.VMEM((tiles, comps, fine_rows, LANES), f32),
            pltpu.VMEM((tiles, comps, fine_rows, LANES), f32),
            pltpu.VMEM((tiles, fine_rows, LANES), f32),
            pltpu.VMEM((comps, 2, 2, halves, padded, LANES), f32),
            pltpu.VMEM((comps, 2, 2, halves, padded, LANES), f32),
            pltpu.VMEM((comps, 2, 2, halves, rows, LANES), f32),
            pltpu.VMEM((2, 2, halves, rows, LANES), f32),
            pltpu.VMEM((2, 2, halves, rows, LANES), f32),
            pltpu.VMEM((comps, rows, width), f32),
            pltpu.VMEM((comps, rows, width), f32),
            pltpu.VMEM((rows, width), f32),
            pltpu.VMEM((comps, halves, padded, LANES), f32),
            pltpu.VMEM((comps, halves, padded, LANES), f32),
            pltpu.VMEM((comps, rows, width), f32),
            pltpu.VMEM((ITERS, 2, halves, SUB, LANES), f32),
            pltpu.VMEM((ITERS, 2, halves, SUB, LANES), f32),
            pltpu.VMEM((ITERS, 2 * SUB, rows), f32),
            pltpu.VMEM((ITERS, LANES, rows), f32),
            pltpu.VMEM((ITERS, 2, halves, SUB, LANES), f32),
            pltpu.VMEM((ITERS, 2, halves, SUB, LANES), f32),
            pltpu.VMEM((ITERS, 2 * SUB, rows), f32),
            pltpu.VMEM((ITERS, LANES, rows), f32),
            pltpu.VMEM((ITERS, 4, SUB, LANES), f32),
            pltpu.VMEM((rows, LANES), f32),
            pltpu.VMEM((padded, LANES), f32),
            pltpu.VMEM((padded, LANES), f32),
            pltpu.VMEM((n_gx, SUB, LANES), f32),
            pltpu.VMEM((n_gy, SUB, LANES), f32),
            dma((3, tiles)),
            dma((tiles,)),
            dma((3,)),
            dma((3, n_gy)),
            dma((3, n_gy)),
            dma((ITERS, 4)),
            dma((ITERS, 4)),
            dma((ITERS, 8)),
            dma((ITERS, 8)),
            dma((1,)),
            dma((n_gy,)),
            dma((n_gy,)),
            dma((n_gx,)),
            dma((n_gx,)),
            dma((n_gy,)),
            dma((n_gy,)),
        ],
        compiler_params=pltpu.CompilerParams(
            collective_id=0, has_side_effects=True, vmem_limit_bytes=48 * 1024 * 1024
        ),
    )(fine_start, fine_known, fine_mu, coarse_start, coarse_known, coarse_mu)
    return fine_ghost, coarse_ghost, norms[:ITERS, 0]


def solution(mesh):
    n_gx, n_gy = mesh.shape["gx"], mesh.shape["gy"]
    return jax.shard_map(
        functools.partial(on_device, n_gx, n_gy),
        mesh=mesh,
        in_specs=(
            P(None, "gx", "gy"),
            P(None, "gx", "gy"),
            P("gx", "gy"),
            P(None, ("gx", "gy"), None),
            P(None, ("gx", "gy"), None),
            P(("gx", "gy"), None),
        ),
        out_specs=(P(None, "gx", "gy"), P(None, ("gx", "gy"), None), P()),
        check_vma=False,
    )
```

```python
import functools

import jax
import jax.numpy as jnp
from jax import lax
from jax.experimental import pallas as pl
from jax.experimental.pallas import tpu as pltpu
from jax.sharding import PartitionSpec as P

ITERS = 3
LANES = 128
SUB = 8
UNROLL = 2
MESH = pl.DeviceIdType.MESH
DIRECTIONS = ((-1, 0), (1, 0), (0, -1), (0, 1), (-1, -1), (1, 1), (-1, 1), (1, -1))


def lane_index():
    return lax.broadcasted_iota(jnp.int32, (SUB, LANES), 1)


def roll_lanes(cells, shift):
    shift = shift % LANES
    return cells if shift == 0 else pltpu.roll(cells, shift, 1)


def from_left(halves, halo):
    first = lane_index() == 0
    rolled = [roll_lanes(cells, 1) for cells in halves]
    return [jnp.where(first, before, own) for before, own in zip([halo] + rolled[:-1], rolled)]


def from_right(halves, halo):
    last = lane_index() == LANES - 1
    rolled = [roll_lanes(cells, LANES - 1) for cells in halves]
    return [jnp.where(last, after, own) for own, after in zip(rolled, rolled[1:] + [halo])]


def kernel(
    n_gx,
    n_gy,
    cells_total,
    fine_start,
    fine_known,
    fine_mu,
    coarse_start,
    coarse_known,
    coarse_mu,
    fine_out,
    coarse_out,
    norms_out,
    raw_start,
    raw_known,
    raw_mu,
    fine_a,
    fine_b,
    known,
    diag,
    inverse,
    patch_start,
    patch_known,
    patch_mu,
    coarse_a,
    coarse_b,
    patch_out,
    fine_row_send,
    fine_row_recv,
    fine_col_send,
    fine_col_recv,
    row_send,
    row_recv,
    col_send,
    col_recv,
    corner_recv,
    packed,
    fine_halo,
    coarse_halo,
    norm_x,
    norm_y,
    load_sem,
    store_sem,
    own_sem,
    move_send,
    move_recv,
    fine_send,
    fine_recv,
    halo_send,
    halo_recv,
    back_own,
    back_send,
    back_recv,
    normx_send,
    normx_recv,
    normy_send,
    normy_recv,
):
    gx = lax.axis_index("gx")
    gy = lax.axis_index("gy")
    fine, coarse = (fine_a, fine_b), (coarse_a, coarse_b)
    comps, rows, width = patch_start.shape
    halves = width // LANES
    blocks = rows // SUB
    own_rows = coarse_start.shape[1]
    lane = lane_index()

    loads = []
    for which, (source, target) in enumerate(
        ((fine_start, raw_start), (fine_mu, raw_mu), (fine_known, raw_known))
    ):
        for tile in range(2 * halves):
            at = pl.ds(tile * LANES, LANES)
            view = source.at[:, at] if len(source.shape) == 2 else source.at[:, :, at]
            loads.append(
                pltpu.make_async_copy(view, target.at[tile], load_sem.at[which, tile])
            )
    for copy in loads:
        copy.start()

    for ref in (fine_row_recv, fine_col_recv, row_recv, col_recv, corner_recv, row_send, fine_row_send):
        ref[...] = jnp.zeros_like(ref)

    barrier = pltpu.get_barrier_semaphore()

    def greet_gy(step, carry):
        pl.semaphore_signal(
            barrier, inc=1, device_id={"gy": lax.rem(gy + step, n_gy)}, device_id_type=MESH
        )
        return carry

    def greet_gx(step, carry):
        pl.semaphore_signal(
            barrier, inc=1, device_id={"gx": lax.rem(gx + step, n_gx)}, device_id_type=MESH
        )
        return carry

    lax.fori_loop(1, n_gy, greet_gy, 0)
    lax.fori_loop(1, n_gx, greet_gx, 0)

    def inside(direction):
        dx, dy = DIRECTIONS[direction]
        checks = []
        if dx:
            checks.append(gx > 0 if dx < 0 else gx < n_gx - 1)
        if dy:
            checks.append(gy > 0 if dy < 0 else gy < n_gy - 1)
        return functools.reduce(jnp.logical_and, checks)

    for direction in range(4, 8):
        dx, dy = DIRECTIONS[direction]

        @pl.when(inside(direction))
        def _():
            pl.semaphore_signal(
                barrier, inc=1, device_id={"gx": gx + dx, "gy": gy + dy}, device_id_type=MESH
            )

    sides_x = (gx > 0).astype(jnp.int32) + (gx < n_gx - 1).astype(jnp.int32)
    sides_y = (gy > 0).astype(jnp.int32) + (gy < n_gy - 1).astype(jnp.int32)
    pl.semaphore_wait(barrier, n_gy - 1 + n_gx - 1 + sides_x * sides_y)

    moved = ((coarse_start, patch_start), (coarse_known, patch_known), (coarse_mu, patch_mu))

    def move(which, owner, place, sem):
        source, target = moved[which]
        columns = pl.ds(pl.multiple_of(owner * width, LANES), width)
        lines = pl.ds(pl.multiple_of(place * own_rows, SUB), own_rows)
        if len(source.shape) == 2:
            return source.at[:, columns], target.at[lines, :]
        return source.at[:, :, columns], target.at[:, lines, :]

    def own_move(which):
        source, target = move(which, gy, gy, None)
        return pltpu.make_async_copy(source, target, own_sem.at[which])

    def peer_move(which, step):
        peer = lax.rem(gy + step, n_gy)
        source, target = move(which, peer, gy, None)
        return pltpu.make_async_remote_copy(
            source,
            target,
            move_send.at[which, step],
            move_recv.at[which, step],
            device_id={"gy": peer},
            device_id_type=MESH,
        )

    def wait_moves(which):
        own_move(which).wait()

        def body(step, carry):
            peer = lax.rem(gy + n_gy - step, n_gy)
            source, target = move(which, gy, peer, None)
            pltpu.make_async_remote_copy(
                source,
                target,
                move_send.at[which, step],
                move_recv.at[which, step],
                device_id={"gy": lax.rem(gy + step, n_gy)},
                device_id_type=MESH,
            ).wait()
            return carry

        lax.fori_loop(1, n_gy, body, 0)

    def send_moves(which):
        def body(step, carry):
            peer_move(which, step).start()
            return carry

        lax.fori_loop(1, n_gy, body, 0)
        own_move(which).start()

    send_moves(0)

    half_lane = lane < LANES // 2
    evens_first = jnp.where(half_lane, 2 * lane, 2 * lane - LANES + 1)
    odds_first = jnp.where(half_lane, 2 * lane + 1, 2 * lane - LANES)

    def split_columns(a, b):
        a = jnp.take_along_axis(a, evens_first, axis=1)
        b = jnp.take_along_axis(b, odds_first, axis=1)
        return (
            jnp.where(half_lane, a, b),
            pltpu.roll(jnp.where(half_lane, b, a), LANES // 2, 1),
        )

    def split_field(raw, put):
        def body(block, carry):
            out = []
            for comp in range(comps):
                for parity in range(2):
                    for half in range(halves):
                        at = pl.ds(block * 2 * SUB + parity, SUB, stride=2)
                        both = split_columns(
                            raw[2 * half, comp, at, :], raw[2 * half + 1, comp, at, :]
                        )
                        out.append((comp, parity, half, both))
            for comp, parity, half, both in out:
                put(comp, parity, 0, half, block, both[0])
                put(comp, parity, 1, half, block, both[1])
            return carry

        lax.fori_loop(0, blocks, body, 0)

    def rows_of(block, shift=0):
        if shift == 0:
            return pl.ds(pl.multiple_of(block * SUB + SUB, SUB), SUB)
        return pl.ds(block * SUB + SUB + shift, SUB)

    def plain(block):
        return pl.ds(pl.multiple_of(block * SUB, SUB), SUB)

    def put_start(comp, parity, side, half, block, cells):
        fine[0][comp, parity, side, half, rows_of(block), :] = cells

    def put_known(comp, parity, side, half, block, cells):
        known[comp, parity, side, half, plain(block), :] = cells

    def split_mu(block, carry):
        out = []
        for parity in range(2):
            for half in range(halves):
                at = pl.ds(block * 2 * SUB + parity, SUB, stride=2)
                both = split_columns(raw_mu[2 * half, at, :], raw_mu[2 * half + 1, at, :])
                for side in range(2):
                    total = both[side] + 1.0
                    out.append((parity, side, half, total, 1.0 / total))
        for parity, side, half, total, reciprocal in out:
            diag[parity, side, half, plain(block), :] = total
            inverse[parity, side, half, plain(block), :] = reciprocal
        return carry

    def place_start(block, carry):
        for comp in range(comps):
            for half in range(halves):
                coarse[0][comp, half, rows_of(block), :] = patch_start[
                    comp, plain(block), half * LANES : (half + 1) * LANES
                ]
        return carry

    def pack(edges, target):
        def body(block, carry):
            out = []
            for way, at in ((0, 0), (1, LANES - 1)):
                for k, edge in enumerate(edges(way, block)):
                    out.append((SUB * way + k, roll_lanes(edge, SUB * way + k - at)))
            cells = jnp.zeros((SUB, LANES), jnp.float32)
            for k, edge in out:
                cells = jnp.where(lane == k, edge, cells)
            packed[plain(block), :] = cells
            return carry

        lax.fori_loop(0, blocks, body, 0, unroll=4)
        target[...] = packed[...].T[: 2 * SUB]

    def message(rows_out, rows_in, cols_out, cols_in, sends, recvs, sweep, direction):
        dx, dy = DIRECTIONS[direction]
        way = direction % 2
        if direction < 2:
            source, target = rows_out.at[sweep, way], rows_in.at[sweep, 1 - way]
        elif direction < 4:
            source = cols_out.at[sweep, pl.ds(SUB * way, SUB), :]
            target = cols_in.at[sweep, pl.ds(SUB * (1 - way), SUB), :]
        else:
            half = 0 if dy < 0 else halves - 1
            source = rows_out.at[sweep, 0 if dx < 0 else 1, half]
            target = corner_recv.at[sweep, (direction ^ 1) - 4]
        return pltpu.make_async_remote_copy(
            source,
            target,
            sends.at[sweep, direction],
            recvs.at[sweep, direction ^ 1],
            device_id={"gx": gx + dx, "gy": gy + dy},
            device_id_type=MESH,
        )

    fine_message = functools.partial(
        message, fine_row_send, fine_row_recv, fine_col_send, fine_col_recv, fine_send, fine_recv
    )
    coarse_message = functools.partial(
        message, row_send, row_recv, col_send, col_recv, halo_send, halo_recv
    )

    def start_all(of, sweep, directions):
        for direction in directions:

            @pl.when(inside(direction))
            def _():
                of(sweep, direction).start()

    def wait_all(of, sweep, directions):
        for direction in directions:

            @pl.when(inside(direction))
            def _():
                of(sweep, direction).wait_send()
                of(sweep, direction ^ 1).wait_recv()

    def send_fine(sweep):
        buf = sweep % 2
        for way, line in enumerate((SUB, SUB + rows - 1)):
            for half in range(halves):
                for comp in range(comps):
                    for side in range(2):
                        at = 2 * comp + side
                        fine_row_send[sweep, way, half, at : at + 1, :] = fine[buf][
                            comp, way, side, half, line : line + 1, :
                        ]
        start_all(fine_message, sweep, (0, 1))

        def edges(way, block):
            half = way * (halves - 1)
            return [
                fine[buf][k // 2, k % 2, way, half, rows_of(block), :] for k in range(2 * comps)
            ]

        pack(edges, fine_col_send.at[sweep])
        start_all(fine_message, sweep, (2, 3))

    def take_fine(sweep):
        buf = sweep % 2
        wait_all(fine_message, sweep, range(4))
        for half in range(halves):
            for comp in range(comps):
                for side in range(2):
                    at = 2 * comp + side
                    fine[buf][comp, 1, side, half, SUB - 1 : SUB, :] = fine_row_recv[
                        sweep, 0, half, at : at + 1, :
                    ]
                    fine[buf][comp, 0, side, half, SUB + rows : SUB + rows + 1, :] = (
                        fine_row_recv[sweep, 1, half, at : at + 1, :]
                    )
        fine_halo[SUB : SUB + rows, :] = fine_col_recv[sweep].T

    def send_coarse(sweep):
        buf = sweep % 2
        for way, line in enumerate((SUB, SUB + rows - 1)):
            for half in range(halves):
                for comp in range(comps):
                    row_send[sweep, way, half, comp : comp + 1, :] = coarse[buf][
                        comp, half, line : line + 1, :
                    ]
        start_all(coarse_message, sweep, (4, 5, 6, 7, 0, 1))

        def edges(way, block):
            half = way * (halves - 1)
            return [coarse[buf][k, half, rows_of(block), :] for k in range(comps)]

        pack(edges, col_send.at[sweep])
        start_all(coarse_message, sweep, (2, 3))

    def take_coarse(sweep):
        buf = sweep % 2
        wait_all(coarse_message, sweep, range(8))
        for half in range(halves):
            for comp in range(comps):
                for way, line in enumerate((SUB - 1, SUB + rows)):
                    coarse[buf][comp, half, line : line + 1, :] = row_recv[
                        sweep, way, half, comp : comp + 1, :
                    ]
        coarse_halo[SUB : SUB + rows, :] = col_recv[sweep].T
        corner_lanes = ((0, 2), (3, 1))
        for corners, line in zip(corner_lanes, (SUB - 1, SUB + rows)):
            held = jnp.zeros((SUB, LANES), jnp.float32)
            for way, corner in enumerate(corners):
                block = corner_recv[sweep, corner]
                for comp in range(comps):
                    k = SUB * way + comp
                    lifted = pltpu.roll(block, SUB - comp, 0) if comp else block
                    moved = roll_lanes(lifted, k - (0 if way else LANES - 1))
                    held = jnp.where(lane == k, moved, held)
            coarse_halo[line : line + 1, :] = held[0:1, :]

    def halo_pair(halo, k, lines):
        cells = halo[lines, :]
        return roll_lanes(cells, -k), roll_lanes(cells, LANES - 1 - SUB - k)

    def coarse_pass(buf, last):
        def body(block, totals):
            totals = list(totals)
            lines = plain(block)
            out = []
            scales = [
                patch_mu[lines, half * LANES : (half + 1) * LANES] + 1.0 for half in range(halves)
            ]
            reciprocals = [1.0 / scale for scale in scales]
            for comp in range(comps):
                left, right = halo_pair(coarse_halo, comp, rows_of(block))
                own = [coarse[buf][comp, half, rows_of(block), :] for half in range(halves)]
                lefts, rights = from_left(own, left), from_right(own, right)
                for half in range(halves):
                    columns = slice(half * LANES, (half + 1) * LANES)
                    near = (
                        coarse[buf][comp, half, rows_of(block, 1), :]
                        + coarse[buf][comp, half, rows_of(block, -1), :]
                        + rights[half]
                        + lefts[half]
                    )
                    below = (
                        fine[buf][comp, 0, 0, half, rows_of(block), :]
                        + fine[buf][comp, 1, 0, half, rows_of(block), :]
                        + fine[buf][comp, 0, 1, half, rows_of(block), :]
                        + fine[buf][comp, 1, 1, half, rows_of(block), :]
                    )
                    res = (
                        patch_known[comp, lines, columns]
                        + 0.25 * near
                        + 0.125 * below
                        - scales[half] * own[half]
                    )
                    totals[comp] = totals[comp] + res * res
                    out.append((comp, half, own[half] + res * reciprocals[half]))
            for comp, half, new in out:
                if last:
                    patch_out[comp, lines, half * LANES : (half + 1) * LANES] = new
                else:
                    coarse[1 - buf][comp, half, rows_of(block), :] = new
            return tuple(totals)

        zero = jnp.zeros((SUB, LANES), jnp.float32)
        return sum(lax.fori_loop(0, blocks, body, (zero,) * comps, unroll=UNROLL))

    def fine_pass(buf):
        def body(block, totals):
            totals = list(totals)
            out = []
            for comp in range(comps):
                mid = [coarse[buf][comp, half, rows_of(block), :] for half in range(halves)]
                mid_left, mid_right = halo_pair(coarse_halo, comp, rows_of(block))
                for parity in range(2):
                    shift = 1 if parity else -1
                    far_left, far_right = halo_pair(coarse_halo, comp, rows_of(block, shift))
                    line = [
                        0.75 * mid[half]
                        + 0.25 * coarse[buf][comp, half, rows_of(block, shift), :]
                        for half in range(halves)
                    ]
                    line_left = from_left(line, 0.75 * mid_left + 0.25 * far_left)
                    line_right = from_right(line, 0.75 * mid_right + 0.25 * far_right)
                    fine_left, fine_right = halo_pair(fine_halo, 2 * comp + parity, rows_of(block))
                    evens, odds = (
                        [fine[buf][comp, parity, side, half, rows_of(block), :] for half in range(halves)]
                        for side in range(2)
                    )
                    before, after = from_left(odds, fine_left), from_right(evens, fine_right)
                    for half in range(halves):
                        for side in range(2):
                            own = odds[half] if side else evens[half]
                            lateral = (
                                evens[half] + after[half] if side else odds[half] + before[half]
                            )
                            near = (
                                fine[buf][comp, 1 - parity, side, half, rows_of(block), :]
                                + fine[buf][comp, 1 - parity, side, half, rows_of(block, shift), :]
                                + lateral
                            )
                            spread = 0.75 * line[half] + 0.25 * (
                                line_right[half] if side else line_left[half]
                            )
                            res = (
                                known[comp, parity, side, half, plain(block), :]
                                + 0.25 * near
                                + 0.5 * spread
                                - diag[parity, side, half, plain(block), :] * own
                            )
                            totals[comp] = totals[comp] + res * res
                            new = own + res * inverse[parity, side, half, plain(block), :]
                            out.append((comp, parity, side, half, new))
            for comp, parity, side, half, new in out:
                fine[1 - buf][comp, parity, side, half, rows_of(block), :] = new
            return tuple(totals)

        zero = jnp.zeros((SUB, LANES), jnp.float32)
        return sum(lax.fori_loop(0, blocks, body, (zero,) * comps))

    def back_place(owner, place):
        return (
            patch_out.at[:, pl.ds(pl.multiple_of(owner * own_rows, SUB), own_rows), :],
            coarse_out.at[:, :, pl.ds(pl.multiple_of(place * width, LANES), width)],
        )

    def back_move(step, place_step):
        peer = lax.rem(gy + step, n_gy)
        source, _ = back_place(peer, gy)
        _, target = back_place(peer, lax.rem(gy + place_step, n_gy))
        return pltpu.make_async_remote_copy(
            source,
            target,
            back_send.at[step],
            back_recv.at[step],
            device_id={"gy": peer},
            device_id_type=MESH,
        )

    def back_start(step, carry):
        back_move(step, 0).start()
        return carry

    def back_wait(step, carry):
        back_move(step, n_gy - step).wait()
        return carry

    own_back = pltpu.make_async_copy(*back_place(gy, gy), back_own.at[0])
    row = lax.broadcasted_iota(jnp.int32, (SUB, LANES), 0)
    totals = [None] * ITERS
    tiles = 2 * halves
    for copy in loads[:tiles]:
        copy.wait()
    split_field(raw_start, put_start)
    send_fine(0)
    send_moves(2)
    for copy in loads[tiles : 2 * tiles]:
        copy.wait()
    lax.fori_loop(0, blocks, split_mu, 0, unroll=2)
    for copy in loads[2 * tiles :]:
        copy.wait()
    split_field(raw_known, put_known)
    wait_moves(0)
    lax.fori_loop(0, blocks, place_start, 0, unroll=4)
    send_coarse(0)
    send_moves(1)
    take_fine(0)
    take_coarse(0)

    totals[0] = fine_pass(0)
    send_fine(1)
    wait_moves(2)
    wait_moves(1)
    totals[0] = totals[0] + coarse_pass(0, False)
    for sweep in range(1, ITERS):
        buf = sweep % 2
        last = sweep == ITERS - 1
        if sweep == 1:
            send_coarse(1)
        take_coarse(sweep)
        totals[sweep] = coarse_pass(buf, last)
        if last:
            lax.fori_loop(1, n_gy, back_start, 0)
            own_back.start()
        else:
            send_coarse(sweep + 1)
        take_fine(sweep)
        totals[sweep] = totals[sweep] + fine_pass(buf)
        if not last:
            send_fine(sweep + 1)
    sums = jnp.zeros((SUB, LANES), jnp.float32)
    for sweep in range(ITERS):
        sums = jnp.where(row == sweep, jnp.sum(totals[sweep], axis=0, keepdims=True), sums)

    def spread_sum(slots, axis, me, count, send_sems, recv_sems, between):
        def message(step, place_step):
            peer = lax.rem(me + step, count)
            return pltpu.make_async_remote_copy(
                slots.at[me],
                slots.at[lax.rem(me + place_step, count)],
                send_sems.at[step],
                recv_sems.at[step],
                device_id={axis: peer},
                device_id_type=MESH,
            )

        def start(step, carry):
            message(step, 0).start()
            return carry

        def wait(step, carry):
            message(step, count - step).wait()
            return carry

        lax.fori_loop(1, count, start, 0)
        between()
        lax.fori_loop(1, count, wait, 0)
        return lax.fori_loop(
            0, count, lambda i, acc: acc + slots[i], jnp.zeros((SUB, LANES), jnp.float32)
        )

    final = ITERS % 2
    weave_a = jnp.where(lane % 2 == 0, lane // 2, lane // 2 + LANES // 2)
    weave_b = jnp.where(lane % 2 == 0, lane // 2 + LANES // 2, lane // 2)

    def weave(block, carry):
        out = []
        for comp in range(comps):
            for parity in range(2):
                for half in range(halves):
                    even = fine[final][comp, parity, 0, half, rows_of(block), :]
                    odd = fine[final][comp, parity, 1, half, rows_of(block), :]
                    odd = pltpu.roll(odd, LANES // 2, 1)
                    at = pl.ds(block * 2 * SUB + parity, SUB, stride=2)
                    a = jnp.take_along_axis(jnp.where(half_lane, even, odd), weave_a, axis=1)
                    b = jnp.take_along_axis(jnp.where(half_lane, odd, even), weave_b, axis=1)
                    out.append((2 * half, comp, at, a))
                    out.append((2 * half + 1, comp, at, b))
        for tile, comp, at, cells in out:
            raw_start[tile, comp, at, :] = cells
        return carry

    stores = [
        pltpu.make_async_copy(
            raw_start.at[tile],
            fine_out.at[:, :, pl.ds(tile * LANES, LANES)],
            store_sem.at[tile],
        )
        for tile in range(tiles)
    ]

    def put_fine():
        lax.fori_loop(0, blocks, weave, 0)
        for copy in stores:
            copy.start()

    norm_x[gx] = sums
    partial = spread_sum(norm_x, "gx", gx, n_gx, normx_send, normx_recv, put_fine)
    norm_y[gy] = partial
    whole = spread_sum(norm_y, "gy", gy, n_gy, normy_send, normy_recv, lambda: None)
    root = jnp.sqrt(jnp.sum(whole, axis=1, keepdims=True) / cells_total)
    norms_out[...] = jnp.broadcast_to(root, norms_out.shape)

    for copy in stores:
        copy.wait()
    own_back.wait()
    lax.fori_loop(1, n_gy, back_wait, 0)


def on_device(n_gx, n_gy, fine_start, fine_known, fine_mu, coarse_start, coarse_known, coarse_mu):
    comps, fine_rows, fine_cols = fine_start.shape
    rows, width = fine_rows // 2, fine_cols // 2
    halves = width // LANES
    tiles = 2 * halves
    padded = rows + 2 * SUB
    cells_total = 3.0 * (fine_mu.size + coarse_mu.size) * n_gx * n_gy
    f32 = jnp.float32
    dma = pltpu.SemaphoreType.DMA
    anywhere = pl.BlockSpec(memory_space=pl.ANY)
    fine_ghost, coarse_ghost, norms = pl.pallas_call(
        functools.partial(kernel, n_gx, n_gy, cells_total),
        out_shape=(
            jax.ShapeDtypeStruct(fine_start.shape, f32),
            jax.ShapeDtypeStruct(coarse_start.shape, f32),
            jax.ShapeDtypeStruct((SUB, LANES), f32),
        ),
        in_specs=[pl.BlockSpec(memory_space=pltpu.HBM)] * 6,
        out_specs=(anywhere, anywhere, pl.BlockSpec(memory_space=pltpu.VMEM)),
        scratch_shapes=[
            pltpu.VMEM((tiles, comps, fine_rows, LANES), f32),
            pltpu.VMEM((tiles, comps, fine_rows, LANES), f32),
            pltpu.VMEM((tiles, fine_rows, LANES), f32),
            pltpu.VMEM((comps, 2, 2, halves, padded, LANES), f32),
            pltpu.VMEM((comps, 2, 2, halves, padded, LANES), f32),
            pltpu.VMEM((comps, 2, 2, halves, rows, LANES), f32),
            pltpu.VMEM((2, 2, halves, rows, LANES), f32),
            pltpu.VMEM((2, 2, halves, rows, LANES), f32),
            pltpu.VMEM((comps, rows, width), f32),
            pltpu.VMEM((comps, rows, width), f32),
            pltpu.VMEM((rows, width), f32),
            pltpu.VMEM((comps, halves, padded, LANES), f32),
            pltpu.VMEM((comps, halves, padded, LANES), f32),
            pltpu.VMEM((comps, rows, width), f32),
            pltpu.VMEM((ITERS, 2, halves, SUB, LANES), f32),
            pltpu.VMEM((ITERS, 2, halves, SUB, LANES), f32),
            pltpu.VMEM((ITERS, 2 * SUB, rows), f32),
            pltpu.VMEM((ITERS, LANES, rows), f32),
            pltpu.VMEM((ITERS, 2, halves, SUB, LANES), f32),
            pltpu.VMEM((ITERS, 2, halves, SUB, LANES), f32),
            pltpu.VMEM((ITERS, 2 * SUB, rows), f32),
            pltpu.VMEM((ITERS, LANES, rows), f32),
            pltpu.VMEM((ITERS, 4, SUB, LANES), f32),
            pltpu.VMEM((rows, LANES), f32),
            pltpu.VMEM((padded, LANES), f32),
            pltpu.VMEM((padded, LANES), f32),
            pltpu.VMEM((n_gx, SUB, LANES), f32),
            pltpu.VMEM((n_gy, SUB, LANES), f32),
            dma((3, tiles)),
            dma((tiles,)),
            dma((3,)),
            dma((3, n_gy)),
            dma((3, n_gy)),
            dma((ITERS, 4)),
            dma((ITERS, 4)),
            dma((ITERS, 8)),
            dma((ITERS, 8)),
            dma((1,)),
            dma((n_gy,)),
            dma((n_gy,)),
            dma((n_gx,)),
            dma((n_gx,)),
            dma((n_gy,)),
            dma((n_gy,)),
        ],
        compiler_params=pltpu.CompilerParams(
            collective_id=0, has_side_effects=True, vmem_limit_bytes=67043328
        ),
    )(fine_start, fine_known, fine_mu, coarse_start, coarse_known, coarse_mu)
    return fine_ghost, coarse_ghost, norms[:ITERS, 0]


def solution(mesh):
    n_gx, n_gy = mesh.shape["gx"], mesh.shape["gy"]
    return jax.shard_map(
        functools.partial(on_device, n_gx, n_gy),
        mesh=mesh,
        in_specs=(
            P(None, "gx", "gy"),
            P(None, "gx", "gy"),
            P("gx", "gy"),
            P(None, ("gx", "gy"), None),
            P(None, ("gx", "gy"), None),
            P(("gx", "gy"), None),
        ),
        out_specs=(P(None, "gx", "gy"), P(None, ("gx", "gy"), None), P()),
        check_vma=False,
    )
```
